32 devices in a mesh: wave: 8 (over z, y), lev: 4 (over x, core).
Axes of the slice: x: 2, y: 2, z: 4, core: 2. Of those that a mesh axis runs over, the one named last changes fastest.
Arguments:
- spectra: bfloat16 [104, 4, 16, 1280], P('wave', None, 'lev'), may hold values from -0.625 to 0.625
- legendre: bfloat16 [104, 16, 1280], P('wave'), may hold values from -0.15625 to 0.15625
- derivative: bfloat16 [104, 16, 1280], P('wave'), may hold values from -0.15625 to 0.15625
- tracer: float32 [16, 16, 2560], P('lev', 'wave'), may hold values from -6 to 6
- limiter_flags: int32 [16, 16, 2560], P('lev', 'wave'), may hold values 0 or 1
- lat_weight: float32 [16], P('wave'), may hold values from 1 to 10
- slot_wave: int32 [104], replicated, may hold values from 0 to 103, each once
Outputs:
- tendency_spectra: float32 [104, 2, 16, 1280], P('wave', None, 'lev')
The draws below stay inside these ranges and needn't reach their ends.
Inputs may be any that keep to these rules, and one draw needn't show every extreme that they name: `slot_wave`: every wavenumber 0 to 103 stands in exactly one slot.
All inputs are finite; a program needn't handle non-finite values. No bound on the sum of `limiter_flags` on one device may be relied on, other than what follows from the above.
Results may differ from the reference program's by a relative error of at most 0.0003.
The reference program's roundings to bfloat16 on the way count: a program that leaves them out, or rounds other values in their place, can miss the bound.
Values may be sent and summed in bfloat16 or wider, within the bound.
No kernel may reach another device: no remote copies, remote signals or barrier semaphores. Data moves between devices by JAX's collectives and lax.ppermute only.
A program may use at most 128 MiB of HBM per device.

```python
import math
import jax
import jax.numpy as jnp
from jax import lax

NDEG = 1280
NLON = 2560
WAVES = 104
LAT = 16
LEV = 16


def set_ends(drawn, own_key, low, top_value):
    dims = drawn.shape
    place = [jax.random.randint(jax.random.fold_in(own_key, axis), (), 0, dims[axis]) for axis in range(len(dims))]
    drawn = drawn.at[tuple(place)].set(low)
    longest = dims.index(max(dims))
    place[longest] = (place[longest] + 1) % dims[longest]
    return drawn.at[tuple(place)].set(top_value)


def level_of(key, dims, shards, least, largest):
    loudness = 1.0
    for dim, parts in shards:
        heights = jax.random.uniform(jax.random.fold_in(jax.random.fold_in(key, 6), dim), (parts,), jnp.float32, least / len(shards), largest / len(shards))
        loudness = loudness * jnp.repeat(jnp.exp(heights), dims[dim] // parts).reshape((-1,) + (1,) * (len(dims) - 1 - dim))
    return loudness


def bell_draw(key, shape, deviation, most, cuts=(), held_as=jnp.bfloat16):
    array = deviation * jax.random.normal(key, shape, jnp.float32)
    if cuts:
        array = array * level_of(key, shape, cuts, -0.22, 0.18)
    return jnp.clip(array, -most, most).astype(held_as)


def setup_inputs(seed: int = 0) -> dict:
    seeds = jax.random.split(jax.random.key(seed), 8)
    return {
        "spectra": bell_draw(seeds[0], (WAVES, 4, LEV, NDEG), (WAVES ** -0.5), 0.625, ((0, 8), (2, 4))),
        "legendre": bell_draw(seeds[1], (WAVES, LAT, NDEG), NDEG ** -0.5, 0.15625, ((0, 8),)),
        "derivative": bell_draw(seeds[2], (WAVES, LAT, NDEG), NDEG ** -0.5, 0.15625, ((0, 8),)),
        "tracer": bell_draw(seeds[3], (LEV, LAT, NLON), 1.0, 6.0, ((0, 4), (1, 8)), jnp.float32),
        "limiter_flags": set_ends((jax.random.randint(seeds[4], (LEV, LAT, NLON), 0, 2) < 1).astype(jnp.int32), jax.random.fold_in(seeds[4], 1), 0, 1),
        "lat_weight": jnp.clip(jnp.exp(math.log(10.0) - 2.3025851 * jax.random.uniform(seeds[5], (LAT,), jnp.float32) ** level_of(seeds[5], (LAT,), ((0, 8),), -0.2, 0.2)), 1.0, 10.0),
        "slot_wave": jax.random.permutation(seeds[6], WAVES).astype(jnp.int32),
    }


diffusivity = 0.15
courant_limit = 0.45

def wave_tables(slot_wave, lon_count):
    longitude = jnp.arange(lon_count, dtype=jnp.int32)
    phase_index = slot_wave[:, None] * longitude[None, :] % lon_count
    angles = 2.0 * math.pi / lon_count * phase_index.astype(jnp.float32)
    cosine = jnp.cos(angles)
    sine_part = jnp.sin(angles)
    doubled = jnp.where(slot_wave == 0, 1.0, 2.0).astype(jnp.float32)[:, None]
    synthesis_table = jnp.stack([doubled * cosine, -doubled * sine_part]).astype(jnp.bfloat16)
    analysis_table = jnp.stack([cosine, -sine_part]).astype(jnp.bfloat16)
    return (synthesis_table, analysis_table)

def combine_winds(legendre_sum, slope_sum, scaled_wave):
    zonal_real = -scaled_wave * legendre_sum[:, 3] - slope_sum[:, 0]
    zonal_imag = scaled_wave * legendre_sum[:, 2] - slope_sum[:, 1]
    merid_real = -scaled_wave * legendre_sum[:, 1] + slope_sum[:, 2]
    merid_imag = scaled_wave * legendre_sum[:, 0] + slope_sum[:, 3]
    return jnp.stack([zonal_real, zonal_imag, merid_real, merid_imag], axis=1).astype(jnp.bfloat16)

def face_terms(zonal_courant, limiter_flags):
    face_speed = 0.5 * (jnp.roll(zonal_courant, 1, axis=2) + zonal_courant)
    magnitude = jnp.abs(face_speed)
    switched = limiter_flags.astype(jnp.float32)
    diffuse = 0.5 * (magnitude - switched * (magnitude - face_speed * face_speed))
    return (face_speed, diffuse)

def tendency_of(padded, face_speed, diffuse, meridional, row_start, level_start, rows_total, levels_total):
    centre = padded[1:-1, 1:-1]
    western = jnp.roll(centre, 1, axis=2)
    flux_east = face_speed * 0.5 * (western + centre) - diffuse * (centre - western)
    southern = padded[1:-1, :-1]
    northern = padded[1:-1, 1:]
    lat_speed = 0.5 * (meridional[1:-1, :-1] + meridional[1:-1, 1:])
    flux_north = lat_speed * 0.5 * (southern + northern) - 0.5 * jnp.abs(lat_speed) * (northern - southern)
    face_index = row_start + jnp.arange(flux_north.shape[1], dtype=jnp.int32)
    open_rows = ((face_index > 0) & (face_index < rows_total)).astype(jnp.float32)
    flux_north = flux_north * open_rows[None, :, None]
    level_index = level_start + jnp.arange(padded.shape[0] - 1, dtype=jnp.int32)
    open_levels = ((level_index > 0) & (level_index < levels_total)).astype(jnp.float32)
    flux_up = diffusivity * (padded[1:, 1:-1] - padded[:-1, 1:-1]) * open_levels[:, None, None]
    return -(jnp.roll(flux_east, -1, axis=2) - flux_east) - (flux_north[:, 1:] - flux_north[:, :-1]) + (flux_up[1:] - flux_up[:-1])

def reference(spectra, legendre, derivative, tracer, limiter_flags, lat_weight, slot_wave):
    degree = jnp.arange(NDEG, dtype=jnp.int32)

    def per_slot(operands):
        coefficients, legendre_row, slope_row, wavenumber = operands
        live_mask = (degree >= wavenumber).astype(coefficients.dtype)
        flattened = (coefficients * live_mask[None, None, :]).reshape(4 * LEV, NDEG)
        legendre_sum = jnp.dot(flattened, legendre_row.T, preferred_element_type=jnp.float32).reshape(1, 4, LEV, LAT)
        slope_sum = jnp.dot(flattened, slope_row.T, preferred_element_type=jnp.float32).reshape(1, 4, LEV, LAT)
        scaled_wave = (wavenumber.astype(jnp.float32) / NDEG).reshape(1, 1, 1)
        return combine_winds(legendre_sum, slope_sum, scaled_wave)[0]
    fourier = lax.map(per_slot, (spectra, legendre, derivative, slot_wave))
    synthesis_table, analysis_table = wave_tables(slot_wave, NLON)
    flipped = fourier.transpose(1, 0, 2, 3).astype(jnp.float32)
    table_wide = synthesis_table.astype(jnp.float32)
    eastward = jnp.einsum('rmkj,rmi->kji', flipped[0:2], table_wide, precision=lax.Precision.HIGHEST)
    northward = jnp.einsum('rmkj,rmi->kji', flipped[2:4], table_wide, precision=lax.Precision.HIGHEST)
    zonal_courant = courant_limit * jnp.tanh(eastward)
    merid_courant = courant_limit * jnp.tanh(northward)
    face_speed, diffuse = face_terms(zonal_courant, limiter_flags)
    widths = ((1, 1), (1, 1), (0, 0))
    merid_padded = jnp.pad(merid_courant, widths)
    section_one = tracer + tendency_of(jnp.pad(tracer, widths), face_speed, diffuse, merid_padded, 0, 0, LAT, LEV)
    section_two = tendency_of(jnp.pad(section_one, widths), face_speed, diffuse, merid_padded, 0, 0, LAT, LEV)
    updated = 0.5 * tracer + 0.5 * (section_one + section_two)
    change = updated - tracer
    lat_scale = lat_weight * (1.0 / math.sqrt(NLON))
    projected = jnp.einsum('kji,rmi->mrkj', change, analysis_table.astype(jnp.float32), precision=lax.Precision.HIGHEST)
    outgoing = projected * lat_scale[None, None, None, :]

    def analyse(operands):
        arrived, legendre_row, wavenumber = operands
        live_mask = (degree >= wavenumber).astype(jnp.float32)
        summed = jnp.dot(arrived.reshape(2 * LEV, LAT), legendre_row.astype(jnp.float32), precision=lax.Precision.HIGHEST)
        return (summed * live_mask[None, :]).reshape(2, LEV, NDEG)
    return lax.map(analyse, (outgoing, legendre, slot_wave))
```

```python
import math

import jax
import jax.numpy as jnp
from jax import lax
from jax.sharding import PartitionSpec as P

diffusivity = 0.15
courant_limit = 0.45
halo = 2


def neighbours(axis):
    count = lax.axis_size(axis)
    forward = [(i, i + 1) for i in range(count - 1)]
    return forward, [(target, source) for source, target in forward]


def wave_table(slot_wave, lon_count):
    longitude = jnp.arange(lon_count, dtype=jnp.int32)
    phase_index = slot_wave[:, None] * longitude[None, :] % lon_count
    angles = 2.0 * math.pi / lon_count * phase_index.astype(jnp.float32)
    return jnp.stack([jnp.cos(angles), -jnp.sin(angles)]).astype(jnp.bfloat16)


def combine_winds(legendre_sum, slope_sum, scaled_wave, doubled):
    zonal_real = -scaled_wave * legendre_sum[:, 3] - slope_sum[:, 0]
    zonal_imag = scaled_wave * legendre_sum[:, 2] - slope_sum[:, 1]
    merid_real = -scaled_wave * legendre_sum[:, 1] + slope_sum[:, 2]
    merid_imag = scaled_wave * legendre_sum[:, 0] + slope_sum[:, 3]
    stacked = jnp.stack([zonal_real, zonal_imag, merid_real, merid_imag], axis=1)
    return (stacked * doubled).astype(jnp.bfloat16)


def face_terms(zonal_courant, switched):
    face_speed = 0.5 * (jnp.roll(zonal_courant, 1, axis=2) + zonal_courant)
    magnitude = jnp.abs(face_speed)
    diffuse = 0.5 * (magnitude - switched * (magnitude - face_speed * face_speed))
    return (face_speed, diffuse)


def tendency_of(
    padded, face_speed, diffuse, meridional, row_start, level_start, rows_total, levels_total
):
    centre = padded[1:-1, 1:-1]
    western = jnp.roll(centre, 1, axis=2)
    flux_east = face_speed * 0.5 * (western + centre) - diffuse * (centre - western)
    southern = padded[1:-1, :-1]
    northern = padded[1:-1, 1:]
    lat_speed = 0.5 * (meridional[1:-1, :-1] + meridional[1:-1, 1:])
    flux_north = lat_speed * 0.5 * (southern + northern) - 0.5 * jnp.abs(lat_speed) * (
        northern - southern
    )
    face_index = row_start + jnp.arange(flux_north.shape[1], dtype=jnp.int32)
    open_rows = ((face_index > 0) & (face_index < rows_total)).astype(jnp.float32)
    flux_north = flux_north * open_rows[None, :, None]
    level_index = level_start + jnp.arange(padded.shape[0] - 1, dtype=jnp.int32)
    open_levels = ((level_index > 0) & (level_index < levels_total)).astype(jnp.float32)
    flux_up = diffusivity * (padded[1:, 1:-1] - padded[:-1, 1:-1]) * open_levels[:, None, None]
    return (
        -(jnp.roll(flux_east, -1, axis=2) - flux_east)
        - (flux_north[:, 1:] - flux_north[:, :-1])
        + (flux_up[1:] - flux_up[:-1])
    )


def exchange_edges(tracer, switched):
    levels, rows, lon_count = tracer.shape
    forward, backward = neighbours("wave")
    north = jnp.concatenate([tracer[:, -2:], switched[:, -1:]], axis=1)
    south = jnp.concatenate([tracer[:, :2], switched[:, :1]], axis=1)
    from_south = lax.ppermute(north, "wave", forward)
    from_north = lax.ppermute(south, "wave", backward)
    rows_ext = jnp.concatenate([from_south[:, :2], tracer, from_north[:, :2]], axis=1)
    flags_ext = jnp.concatenate([from_south[:, 2:], switched, from_north[:, 2:]], axis=1)
    forward, backward = neighbours("lev")

    def packed(edge, inner):
        return jnp.concatenate(
            [rows_ext[edge, 1:-1], rows_ext[inner, 2:-2], switched[edge]], axis=0
        )

    from_below = lax.ppermute(packed(levels - 1, levels - 2), "lev", forward)
    from_above = lax.ppermute(packed(0, 1), "lev", backward)

    def unpacked(got):
        near = jnp.pad(got[: rows + 2], ((1, 1), (0, 0)))
        far = jnp.pad(got[rows + 2 : 2 * rows + 2], ((2, 2), (0, 0)))
        flags = jnp.pad(got[2 * rows + 2 :], ((1, 1), (0, 0)))
        return near[None], far[None], flags[None]

    near_b, far_b, flags_b = unpacked(from_below)
    near_a, far_a, flags_a = unpacked(from_above)
    tracer_ext = jnp.concatenate([far_b, near_b, rows_ext, near_a, far_a], axis=0)
    return tracer_ext, jnp.concatenate([flags_b, flags_ext, flags_a], axis=0)


def on_device(spectra, legendre, derivative, tracer, limiter_flags, lat_weight, slot_wave):
    slot_count = spectra.shape[0]
    level_count = spectra.shape[2]
    degree_count = spectra.shape[3]
    lat_total = legendre.shape[1]
    band_rows = tracer.shape[1]
    lon_count = tracer.shape[2]
    bands = lax.axis_size("wave")
    sets = lax.axis_size("lev")
    assert band_rows >= halo and level_count >= halo
    lev_total = level_count * sets
    band_index = lax.axis_index("wave")
    row_start = band_index * band_rows
    level_start = lax.axis_index("lev") * level_count
    local_wave = lax.dynamic_slice_in_dim(slot_wave, band_index * slot_count, slot_count)
    degree = jnp.arange(degree_count, dtype=jnp.int32)
    live_mask = degree[None, :] >= local_wave[:, None]
    coefficients = (spectra * live_mask[:, None, None, :].astype(spectra.dtype)).reshape(
        slot_count, 4 * level_count, degree_count
    )
    legendre_sum = jnp.einsum(
        "mcn,mln->mcl", coefficients, legendre, preferred_element_type=jnp.float32
    ).reshape(slot_count, 4, level_count, lat_total)
    slope_sum = jnp.einsum(
        "mcn,mln->mcl", coefficients, derivative, preferred_element_type=jnp.float32
    ).reshape(slot_count, 4, level_count, lat_total)
    scaled_wave = (local_wave.astype(jnp.float32) / degree_count)[:, None, None]
    doubled = jnp.where(local_wave == 0, 1.0, 2.0).astype(jnp.float32)[:, None, None, None]
    fourier = combine_winds(legendre_sum, slope_sum, scaled_wave, doubled)
    rimmed = jnp.pad(fourier, ((0, 0), (0, 0), (0, 0), (halo, halo)))
    window = band_rows + 2 * halo
    pieces = jnp.stack([rimmed[..., b * band_rows : b * band_rows + window] for b in range(bands)])
    piece_shape = pieces.shape[1:]
    pieces = jnp.broadcast_to(
        pieces.reshape(bands, 1, -1), (bands, sets, math.prod(piece_shape))
    ).reshape(bands * sets, -1)
    arrived = lax.all_to_all(pieces, ("wave", "lev"), split_axis=0, concat_axis=0, tiled=True)
    table = wave_table(slot_wave, lon_count)
    tracer_ext, flags_ext = exchange_edges(tracer, limiter_flags.astype(jnp.float32))

    arrived = arrived.reshape((bands, sets) + piece_shape)
    arrived = arrived.transpose(3, 0, 2, 1, 4, 5).reshape(
        2, 2, bands * slot_count, lev_total, window
    )
    arrived = jnp.pad(arrived, ((0, 0), (0, 0), (0, 0), (halo, halo), (0, 0)))
    arrived = lax.dynamic_slice_in_dim(arrived, level_start, level_count + 2 * halo, axis=3)
    winds = jnp.einsum("ermkj,rmi->ekji", arrived, table, preferred_element_type=jnp.float32)
    zonal_courant = courant_limit * jnp.tanh(winds[0, 1:-1, 1:-1])
    merid_courant = courant_limit * jnp.tanh(winds[1])
    face_speed, diffuse = face_terms(zonal_courant, flags_ext)
    section_one = tracer_ext[1:-1, 1:-1] + tendency_of(
        tracer_ext,
        face_speed,
        diffuse,
        merid_courant,
        row_start - 1,
        level_start - 1,
        lat_total,
        lev_total,
    )
    section_two = tendency_of(
        section_one,
        face_speed[1:-1, 1:-1],
        diffuse[1:-1, 1:-1],
        merid_courant[1:-1, 1:-1],
        row_start,
        level_start,
        lat_total,
        lev_total,
    )
    updated = 0.5 * tracer + 0.5 * (section_one[1:-1, 1:-1] + section_two)
    change = updated - tracer
    lat_scale = lat_weight * (1.0 / math.sqrt(lon_count))
    projected = jnp.einsum(
        "kji,rmi->mrkj", change, table.astype(jnp.float32), precision=lax.Precision.HIGHEST
    )
    outgoing = projected * lat_scale[None, None, None, :]
    live_float = live_mask.astype(jnp.float32)
    legendre_wide = legendre.astype(jnp.float32)
    summed = jnp.einsum(
        "mrkj,mjn->mrkn",
        lax.all_to_all(outgoing, "wave", split_axis=0, concat_axis=3, tiled=True),
        legendre_wide,
        precision=lax.Precision.HIGHEST,
    )
    return summed * live_float[:, None, None, :]


def solution(mesh):
    return jax.shard_map(
        on_device,
        mesh=mesh,
        in_specs=(
            P("wave", None, "lev", None),
            P("wave", None, None),
            P("wave", None, None),
            P("lev", "wave", None),
            P("lev", "wave", None),
            P("wave"),
            P(),
        ),
        out_specs=P("wave", None, "lev", None),
        check_vma=False,
    )
```

```python
import functools
import math

import jax
import jax.numpy as jnp
import numpy as np
from jax import lax
from jax.experimental import pallas as pl
from jax.experimental.pallas import tpu as pltpu
from jax.sharding import PartitionSpec as P

diffusivity = 0.15
courant_limit = 0.45
halo = 2
lanes = 128
packed_rows = 16


def round_up(value, step):
    return -(-value // step) * step


def contract(left, right, dims):
    return lax.dot_general(left, right, (dims, ((), ())), preferred_element_type=jnp.float32)


def vmem(count):
    return [pl.BlockSpec(memory_space=pltpu.VMEM)] * count


def smem(count):
    return [pl.BlockSpec(memory_space=pltpu.SMEM)] * count


def params(*byte_counts):
    return pltpu.CompilerParams(vmem_limit_bytes=min(60 * 2**20, 6 * 2**20 + sum(byte_counts)))


class Sizes:
    def __init__(self, spectra, legendre, tracer, bands, sets):
        self.slots, _, self.levels, self.degrees = spectra.shape
        self.lats = legendre.shape[1]
        self.rows, self.lon = tracer.shape[1:]
        self.bands, self.sets = bands, sets
        self.slot_pad = round_up(self.slots, packed_rows)
        self.window = self.rows + 2 * halo
        self.deep = self.levels + 2 * halo
        self.half = round_up(2 * self.levels * self.window, lanes // 2)
        self.piece = round_up(2 * self.half, lanes)
        self.stack = round_up(self.window * self.deep, 8)
        self.reply = round_up(2 * self.levels * self.slot_pad, lanes)
        assert self.rows == halo and self.deep == 8 and self.lon % lanes == 0


def piece_lanes(z):
    at = np.arange(z.piece)
    part, rest = at // z.half, at % z.half
    wind, rest = rest // (z.levels * z.window), rest % (z.levels * z.window)
    valid = (part < 2) & (wind < 2)
    return part, wind, rest // z.levels, rest % z.levels, valid


def pack_constants(z):
    part, wind, row, level, valid = piece_lanes(z)
    source = np.arange(z.slots * 4 * z.levels)
    channel = source // z.levels % 4
    pick = (channel[:, None] == wind * 2 + part) & (source[:, None] % z.levels == level) & valid
    gather = np.arange(z.slot_pad)[:, None] == source // (4 * z.levels)
    offset = np.where(valid, row - halo, -(10**6)) - np.arange(z.lats)[:, None]
    return (
        pick.astype(np.float32),
        jnp.asarray(gather, jnp.bfloat16),
        offset.astype(np.int32),
    )


def unpack_constant(z):
    part, wind, row, level, valid = piece_lanes(z)
    height = round_up(2 * z.stack, lanes)
    target = np.arange(2 * height)
    t_part, rest = target // height, target % height
    t_wind, rest = rest // z.stack, rest % z.stack
    t_row, t_deep = rest // z.deep, rest % z.deep
    t_valid = (t_wind < 2) & (t_row < z.window)
    same = (t_part[:, None] == part) & (t_wind[:, None] == wind) & (t_row[:, None] == row)
    same = same & valid & t_valid[:, None]
    own = same & (t_deep[:, None] == level + halo)
    below = same & (t_deep[:, None] == halo - 1) & (level == z.levels - 1)
    above = same & (t_deep[:, None] == halo + z.levels) & (level == 0)
    return jnp.asarray(np.concatenate([own, below, above], axis=1), jnp.bfloat16)


def reply_constants(z):
    at = np.arange(z.reply)
    part, rest = at // (z.levels * z.slot_pad), at % (z.levels * z.slot_pad)
    level, slot = rest // z.slot_pad, rest % z.slot_pad
    source = np.arange(2 * z.slot_pad)
    spread = (source[:, None] // z.slot_pad == part) & (source[:, None] % z.slot_pad == slot)
    pick = np.arange(z.deep)[:, None] == level + halo
    return jnp.asarray(spread, jnp.bfloat16), pick.astype(np.float32)


def legendre_kernel(
    z,
    wave_ref,
    spectra_ref,
    legendre_ref,
    derivative_ref,
    pick_ref,
    gather_ref,
    offset_ref,
    tracer_ref,
    flags_ref,
    pieces_ref,
    north_ref,
    south_ref,
):
    height = 4 * z.levels
    degree = lax.broadcasted_iota(jnp.int32, (height, z.degrees), 1)
    channel = lax.broadcasted_iota(jnp.int32, (height, z.lats), 0) // z.levels
    sign_sum = jnp.where(channel % 2 == 0, -1.0, 1.0)
    sign_slope = jnp.where(channel < 2, -1.0, 1.0)
    winds = []
    for s in range(z.slots):
        wave = wave_ref[s]
        coefficients = spectra_ref[s].reshape(height, z.degrees)
        coefficients = coefficients * jnp.where(degree >= wave, 1.0, 0.0).astype(jnp.bfloat16)
        sums = contract(coefficients, legendre_ref[s], ((1,), (1,)))
        slopes = contract(coefficients, derivative_ref[s], ((1,), (1,)))
        turned = jnp.concatenate(
            [sums[c * z.levels : (c + 1) * z.levels] for c in (3, 2, 1, 0)], axis=0
        )
        scaled = wave.astype(jnp.float32) / z.degrees
        doubled = jnp.where(wave == 0, 1.0, 2.0)
        winds.append((scaled * sign_sum * turned + sign_slope * slopes) * doubled)
    winds = jnp.concatenate(winds, axis=0).astype(jnp.bfloat16)

    def one_band(b, carry):
        choose = jnp.where(offset_ref[...] + b * z.rows == 0, 1.0, 0.0).astype(jnp.bfloat16)
        spread = contract(winds, choose, ((1,), (0,))) * pick_ref[...]
        piece = contract(gather_ref[...], spread.astype(jnp.bfloat16), ((1,), (0,)))
        piece = piece.astype(jnp.bfloat16)
        for l in range(z.sets):
            pieces_ref[b * z.sets + l] = piece
        return carry

    if z.bands <= 16:
        for b in range(z.bands):
            one_band(b, 0)
    else:
        lax.fori_loop(0, z.bands, one_band, 0)

    for j in range(z.rows):
        row = tracer_ref[:, j, :]
        north_ref[j] = row
        south_ref[j] = row
    north_ref[z.rows] = flags_ref[:, z.rows - 1, :].astype(jnp.float32)
    south_ref[z.rows] = flags_ref[:, 0, :].astype(jnp.float32)


def table_kernel(z, wave_ref, table_ref):
    wave = wave_ref[...].astype(jnp.float32)
    height = wave.shape[0]
    chunks = z.lon // lanes
    at = lax.broadcasted_iota(jnp.int32, (height, lanes), 1).astype(jnp.float32)

    def parts(phase):
        phase = phase - jnp.floor(phase * (1.0 / z.lon) + 0.5) * z.lon
        angle = phase * (2.0 * math.pi / z.lon)
        return jnp.cos(angle), jnp.sin(angle)

    fine_cos, fine_sin = parts(wave * at)
    coarse = [parts(wave * ((at + b) * lanes)) for b in range(0, chunks, lanes)]
    for a in range(chunks):
        cos_a = coarse[a // lanes][0][:, a % lanes : a % lanes + 1]
        sin_a = coarse[a // lanes][1][:, a % lanes : a % lanes + 1]
        columns = slice(a * lanes, (a + 1) * lanes)
        table_ref[:height, columns] = (cos_a * fine_cos - sin_a * fine_sin).astype(jnp.bfloat16)
        table_ref[height:, columns] = (-(sin_a * fine_cos + cos_a * fine_sin)).astype(jnp.bfloat16)


def edge_kernel(z, tracer_ref, flags_ref, south_ref, north_ref, up_ref, down_ref):
    for out_ref, near, far in (
        (up_ref, z.levels - 1, z.levels - 2),
        (down_ref, 0, 1),
    ):
        out_ref[0:1] = south_ref[z.rows - 1, near : near + 1]
        out_ref[1 : 1 + z.rows] = tracer_ref[near]
        out_ref[1 + z.rows : 2 + z.rows] = north_ref[0, near : near + 1]
        out_ref[2 + z.rows : 2 + 2 * z.rows] = tracer_ref[far]
        out_ref[2 + 2 * z.rows : 2 + 3 * z.rows] = flags_ref[near].astype(jnp.float32)


def grid_kernel(
    z,
    place_ref,
    weight_ref,
    arrived_ref,
    unpack_ref,
    table_ref,
    tracer_ref,
    flags_ref,
    south_ref,
    north_ref,
    below_ref,
    above_ref,
    spread_ref,
    pick_ref,
    reply_ref,
    q_ref,
    f_ref,
):
    band, level_set = place_ref[0], place_ref[1]
    lat_total = z.bands * z.rows
    lev_total = z.sets * z.levels
    own = slice(halo, halo + z.levels)
    q_ref[...] = jnp.zeros_like(q_ref)
    f_ref[...] = jnp.zeros_like(f_ref)
    for j in range(halo):
        q_ref[j, own] = south_ref[z.rows - halo + j]
        q_ref[halo + z.rows + j, own] = north_ref[j]
    f_ref[0, own] = south_ref[z.rows]
    f_ref[z.rows + 1, own] = north_ref[z.rows]
    for j in range(z.rows):
        q_ref[halo + j, own] = tracer_ref[:, j, :]
        f_ref[1 + j, own] = flags_ref[:, j, :].astype(jnp.float32)
    for got_ref, near, far in ((below_ref, halo - 1, 0), (above_ref, halo + z.levels, z.deep - 1)):
        for j in range(z.rows + 2):
            q_ref[halo - 1 + j, near : near + 1] = got_ref[j : j + 1]
        for j in range(z.rows):
            at = z.rows + 2 + j
            q_ref[halo + j, far : far + 1] = got_ref[at : at + 1]
            at = 2 * z.rows + 2 + j
            f_ref[1 + j, near : near + 1] = got_ref[at : at + 1]

    height = z.bands * z.slot_pad

    def from_set(index):
        return arrived_ref[:, index].reshape(height, z.piece)

    blocks = jnp.concatenate(
        [
            from_set(level_set),
            from_set(jnp.maximum(level_set - 1, 0)),
            from_set(jnp.minimum(level_set + 1, z.sets - 1)),
        ],
        axis=1,
    )
    turned = contract(unpack_ref[...], blocks, ((1,), (1,))).astype(jnp.bfloat16)
    span = turned.shape[0] // 2
    turned = jnp.concatenate([turned[:span], turned[span:]], axis=1)
    winds = contract(turned, table_ref[...], ((1,), (0,)))

    def wind(which, j):
        first = which * z.stack + j * z.deep
        return courant_limit * jnp.tanh(winds[first : first + z.deep])

    zonal = [wind(0, j) for j in range(1, z.rows + 3)]
    merid = [wind(1, j) for j in range(z.window)]

    def west(x):
        return pltpu.roll(x, 1, 1)

    def east(x):
        return pltpu.roll(x, z.lon - 1, 1)

    face = []
    for j in range(z.rows + 2):
        speed = 0.5 * (west(zonal[j]) + zonal[j])
        magnitude = jnp.abs(speed)
        diffuse = 0.5 * (magnitude - f_ref[j] * (magnitude - speed * speed))
        face.append((speed, diffuse))
    lat_face = []
    for j in range(1, z.window):
        index = band * z.rows - halo + j
        is_open = jnp.where((index > 0) & (index < lat_total), 0.5, 0.0).astype(jnp.float32)
        speed = 0.5 * (merid[j - 1] + merid[j])
        lat_face.append((speed * is_open, jnp.abs(speed) * is_open))
    deep = lax.broadcasted_iota(jnp.int32, (z.deep, z.lon), 0) + (level_set * z.levels - halo)
    rise = jnp.where((deep > 0) & (deep < lev_total), diffusivity, 0.0).astype(jnp.float32)

    def tendency(q, first):
        north_flux = []
        for j in range(len(q) - 1):
            mean, spread = lat_face[first - 1 + j]
            north_flux.append(mean * (q[j] + q[j + 1]) - spread * (q[j + 1] - q[j]))
        result = []
        for j in range(1, len(q) - 1):
            speed, diffuse = face[first - 2 + j]
            centre = q[j]
            western = west(centre)
            flux = speed * 0.5 * (western + centre) - diffuse * (centre - western)
            lift = rise * (centre - pltpu.roll(centre, 1, 0))
            result.append(
                -(east(flux) - flux)
                - (north_flux[j] - north_flux[j - 1])
                + (pltpu.roll(lift, z.deep - 1, 0) - lift)
            )
        return result

    tracer = [q_ref[j] for j in range(z.window)]
    first_tendency = tendency(tracer, 1)
    section_one = [q + t for q, t in zip(tracer[1:-1], first_tendency)]
    section_two = tendency(section_one, 2)
    tops, lows = [], []
    for j in range(z.rows):
        q = tracer[halo + j]
        change = 0.5 * q + 0.5 * (section_one[1 + j] + section_two[j]) - q
        top = change.astype(jnp.bfloat16)
        tops.append(top.astype(jnp.float32))
        lows.append(change - tops[-1])
    both = jnp.concatenate(tops + lows, axis=0).astype(jnp.bfloat16)
    projected = contract(both, table_ref[...], ((1,), (1,)))
    count = z.rows * z.deep
    projected = projected[:count] + projected[count:]
    scaled = []
    for j in range(z.rows):
        scale = weight_ref[j] * (1.0 / math.sqrt(z.lon))
        scaled.append(projected[j * z.deep : (j + 1) * z.deep] * scale)
    scaled = jnp.concatenate(scaled, axis=0)
    top = scaled.astype(jnp.bfloat16)
    low = (scaled - top.astype(jnp.float32)).astype(jnp.bfloat16)
    both = jnp.concatenate([top, low], axis=0)
    for b in range(z.bands):
        first = b * z.slot_pad
        block = jnp.concatenate(
            [both[:, p * height + first : p * height + first + z.slot_pad] for p in range(2)], axis=1
        )
        block = contract(block, spread_ref[...], ((1,), (0,)))
        block = block[:count] + block[count:]
        for j in range(z.rows):
            mine = block[j * z.deep : (j + 1) * z.deep] * pick_ref[...]
            reply_ref[b, j : j + 1] = jnp.sum(mine, axis=0, keepdims=True)


def analysis_kernel(z, wave_ref, arrived_ref, legendre_ref, out_ref, turned_ref):
    arrived = arrived_ref[...].reshape(z.lats, z.reply)
    top = arrived.astype(jnp.bfloat16).astype(jnp.float32)
    turned = jnp.concatenate([top, arrived - top], axis=0)
    width = turned_ref.shape[2]
    for c in range(turned_ref.shape[0]):
        turned_ref[c] = turned[c * width : (c + 1) * width].T
    height = 2 * z.levels
    degree = lax.broadcasted_iota(jnp.int32, (height, z.degrees), 1)
    for s in range(z.slots):
        left = [
            turned_ref[c, pl.ds(s, height, stride=z.slot_pad), :].astype(jnp.bfloat16)
            for c in range(turned_ref.shape[0])
        ]
        left = jnp.concatenate(left, axis=1)
        right = jnp.concatenate([legendre_ref[s], legendre_ref[s]], axis=0)
        summed = contract(left, right, ((1,), (0,)))
        summed = jnp.where(degree >= wave_ref[s], summed, 0.0)
        out_ref[s] = summed.reshape(2, z.levels, z.degrees)


def nbytes(array, dtype=None):
    return array.size * jnp.dtype(dtype or array.dtype).itemsize


def neighbours(axis):
    count = lax.axis_size(axis)
    forward = [(i, i + 1) for i in range(count - 1)]
    return forward, [(target, source) for source, target in forward]


def on_device(spectra, legendre, derivative, tracer, limiter_flags, lat_weight, slot_wave):
    z = Sizes(spectra, legendre, tracer, lax.axis_size("wave"), lax.axis_size("lev"))
    band_index = lax.axis_index("wave")
    place = jnp.stack([band_index, lax.axis_index("lev")]).astype(jnp.int32)
    local_wave = lax.dynamic_slice_in_dim(slot_wave, band_index * z.slots, z.slots)
    f32 = jnp.float32
    fan = 4 * z.bands * z.sets * z.slot_pad * z.piece
    table_bytes = 4 * z.bands * z.slot_pad * z.lon
    edge_shape = jax.ShapeDtypeStruct((z.rows + 1, z.levels, z.lon), f32)
    pieces, to_north, to_south = pl.pallas_call(
        functools.partial(legendre_kernel, z),
        name="legendre",
        in_specs=smem(1) + vmem(8),
        out_specs=tuple(vmem(3)),
        out_shape=(
            jax.ShapeDtypeStruct((z.bands * z.sets, z.slot_pad, z.piece), jnp.bfloat16),
            edge_shape,
            edge_shape,
        ),
        compiler_params=params(2 * nbytes(spectra), 2 * nbytes(legendre), 4 * nbytes(tracer), fan),
    )(
        local_wave,
        spectra,
        legendre,
        derivative,
        *pack_constants(z),
        tracer,
        limiter_flags,
    )
    arrived = lax.all_to_all(pieces, ("wave", "lev"), split_axis=0, concat_axis=0, tiled=True)
    padded_wave = jnp.pad(
        slot_wave.reshape(z.bands, z.slots), ((0, 0), (0, z.slot_pad - z.slots))
    ).reshape(-1, 1)
    table = pl.pallas_call(
        functools.partial(table_kernel, z),
        name="table",
        in_specs=vmem(1),
        out_specs=vmem(1)[0],
        out_shape=jax.ShapeDtypeStruct((2 * z.bands * z.slot_pad, z.lon), jnp.bfloat16),
        compiler_params=params(table_bytes),
    )(padded_wave)
    forward, backward = neighbours("wave")
    from_south = lax.ppermute(to_north, "wave", forward)
    from_north = lax.ppermute(to_south, "wave", backward)
    up_shape = jax.ShapeDtypeStruct((3 * z.rows + 2, z.lon), f32)
    up, down = pl.pallas_call(
        functools.partial(edge_kernel, z),
        name="edges",
        in_specs=vmem(4),
        out_specs=tuple(vmem(2)),
        out_shape=(up_shape, up_shape),
        compiler_params=params(8 * nbytes(tracer)),
    )(tracer, limiter_flags, from_south, from_north)
    forward, backward = neighbours("lev")
    from_below = lax.ppermute(up, "lev", forward)
    from_above = lax.ppermute(down, "lev", backward)
    reply = pl.pallas_call(
        functools.partial(grid_kernel, z),
        name="grid",
        in_specs=smem(2) + vmem(11),
        out_specs=vmem(1)[0],
        out_shape=jax.ShapeDtypeStruct((z.bands, z.rows, z.reply), f32),
        scratch_shapes=[
            pltpu.VMEM((z.window, z.deep, z.lon), f32),
            pltpu.VMEM((z.rows + 2, z.deep, z.lon), f32),
        ],
        compiler_params=params(3 * table_bytes, 24 * nbytes(tracer), fan),
    )(
        place,
        lat_weight,
        arrived.reshape(z.bands, z.sets, z.slot_pad, z.piece),
        unpack_constant(z),
        table,
        tracer,
        limiter_flags,
        from_south,
        from_north,
        from_below,
        from_above,
        *reply_constants(z),
    )
    returned = lax.all_to_all(reply, "wave", split_axis=0, concat_axis=0, tiled=True)
    width = math.gcd(2 * z.lats, lanes)
    return pl.pallas_call(
        functools.partial(analysis_kernel, z),
        name="analysis",
        in_specs=smem(1) + vmem(2),
        out_specs=vmem(1)[0],
        out_shape=jax.ShapeDtypeStruct((z.slots, 2, z.levels, z.degrees), f32),
        scratch_shapes=[pltpu.VMEM((2 * z.lats // width, z.reply, width), f32)],
        compiler_params=params(nbytes(spectra, f32), nbytes(legendre)),
    )(local_wave, returned, legendre)


def solution(mesh):
    return jax.shard_map(
        on_device,
        mesh=mesh,
        in_specs=(
            P("wave", None, "lev", None),
            P("wave", None, None),
            P("wave", None, None),
            P("lev", "wave", None),
            P("lev", "wave", None),
            P("wave"),
            P(),
        ),
        out_specs=P("wave", None, "lev", None),
        check_vma=False,
    )
```

```python
import functools
import math

import jax
import jax.numpy as jnp
import numpy as np
from jax import lax
from jax.experimental import pallas as pl
from jax.experimental.pallas import tpu as pltpu
from jax.sharding import PartitionSpec as P

diffusivity = 0.15
courant_limit = 0.45
halo = 2
lanes = 128
packed_rows = 16
group_slots = 8


def round_up(value, step):
    return -(-value // step) * step


def contract(left, right, dims):
    return lax.dot_general(left, right, (dims, ((), ())), preferred_element_type=jnp.float32)


def vmem(count):
    return [pl.BlockSpec(memory_space=pltpu.VMEM)] * count


def params(*byte_counts):
    return pltpu.CompilerParams(vmem_limit_bytes=min(60 * 2**20, 6 * 2**20 + sum(byte_counts)))


class Sizes:
    def __init__(self, spectra, legendre, tracer, bands, sets):
        self.slots, _, self.levels, self.degrees = spectra.shape
        self.lats = legendre.shape[1]
        self.rows, self.lon = tracer.shape[1:]
        self.bands, self.sets = bands, sets
        self.slot_pad = round_up(self.slots, packed_rows)
        self.window = self.rows + 2 * halo
        self.deep = self.levels + 2 * halo
        self.half = round_up(2 * self.levels * self.window, lanes // 2)
        self.piece = round_up(2 * self.half, lanes)
        self.stack = round_up(self.window * self.deep, 8)
        self.reply = round_up(2 * self.levels * self.slot_pad, lanes)
        assert self.rows == halo and self.deep == 8 and self.lon % lanes == 0


def piece_lanes(z):
    at = np.arange(z.piece)
    part, rest = at // z.half, at % z.half
    wind, rest = rest // (z.levels * z.window), rest % (z.levels * z.window)
    valid = (part < 2) & (wind < 2)
    return part, wind, rest // z.levels, rest % z.levels, valid


def pack_constants(z):
    part, wind, row, level, valid = piece_lanes(z)
    source = np.arange(z.slots * 4 * z.levels)
    channel = source // z.levels % 4
    pick = (channel[:, None] == wind * 2 + part) & (source[:, None] % z.levels == level) & valid
    gather = np.arange(z.slot_pad)[:, None] == source // (4 * z.levels)
    offset = np.where(valid, row - halo, -(10**6)) - np.arange(z.lats)[:, None]
    return (
        pick.astype(np.float32),
        jnp.asarray(gather, jnp.bfloat16),
        offset.astype(np.int32),
    )


def unpack_constant(z):
    part, wind, row, level, valid = piece_lanes(z)
    height = round_up(2 * z.stack, lanes)
    target = np.arange(2 * height)
    t_part, rest = target // height, target % height
    t_wind, rest = rest // z.stack, rest % z.stack
    t_row, t_deep = rest // z.deep, rest % z.deep
    t_valid = (t_wind < 2) & (t_row < z.window)
    same = (t_part[:, None] == part) & (t_wind[:, None] == wind) & (t_row[:, None] == row)
    same = same & valid & t_valid[:, None]
    own = same & (t_deep[:, None] == level + halo)
    below = same & (t_deep[:, None] == halo - 1) & (level == z.levels - 1)
    above = same & (t_deep[:, None] == halo + z.levels) & (level == 0)
    return jnp.asarray(np.concatenate([own, below, above], axis=1), jnp.bfloat16)


def reply_constants(z):
    at = np.arange(z.reply)
    part, rest = at // (z.levels * z.slot_pad), at % (z.levels * z.slot_pad)
    level, slot = rest // z.slot_pad, rest % z.slot_pad
    source = np.arange(2 * z.slot_pad)
    spread = (source[:, None] // z.slot_pad == part) & (source[:, None] % z.slot_pad == slot)
    pick = np.arange(z.deep)[:, None] == level + halo
    return jnp.asarray(spread, jnp.bfloat16), pick.astype(np.float32)


def pack_kernel(z, tracer_hbm, flags_hbm, own_ref, first_ref, second_ref, tracer_ref, flags_ref, sems):
    copies = [
        pltpu.make_async_copy(tracer_hbm, tracer_ref, sems.at[0]),
        pltpu.make_async_copy(flags_hbm, flags_ref, sems.at[1]),
    ]
    for copy in copies:
        copy.start()
    even = lax.axis_index("wave") % 2 == 0
    copies[0].wait()
    for j in range(z.rows):
        row = tracer_ref[:, j, :]
        own_ref[j] = row
        first_ref[j] = row
        second_ref[j] = row
    copies[1].wait()
    switched = [flags_ref[:, j, :].astype(jnp.float32) for j in range(z.rows)]
    for j in range(z.rows):
        own_ref[z.rows + j] = switched[j]
    first_ref[z.rows] = jnp.where(even, switched[-1], switched[0])
    second_ref[z.rows] = jnp.where(even, switched[0], switched[-1])


def legendre_kernel(
    z,
    wave_hbm,
    weight_hbm,
    spectra_hbm,
    legendre_hbm,
    derivative_hbm,
    pick_hbm,
    gather_hbm,
    offset_hbm,
    pieces_ref,
    live_ref,
    scale_ref,
    wave_ref,
    weight_ref,
    spectra_ref,
    legendre_ref,
    derivative_ref,
    pick_ref,
    gather_ref,
    offset_ref,
    sems,
):
    groups = [
        (first, min(first + group_slots, z.slots)) for first in range(0, z.slots, group_slots)
    ]
    fetches = []
    for g, (first, last) in enumerate(groups):
        part = pl.ds(first, last - first)
        fetches.append(
            [
                pltpu.make_async_copy(hbm.at[part], ref.at[part], sems.at[a, g])
                for a, (hbm, ref) in enumerate(
                    (
                        (spectra_hbm, spectra_ref),
                        (legendre_hbm, legendre_ref),
                        (derivative_hbm, derivative_ref),
                    )
                )
            ]
        )
    constants = [
        pltpu.make_async_copy(hbm, ref, sems.at[3 + a, 0])
        for a, (hbm, ref) in enumerate(
            ((pick_hbm, pick_ref), (gather_hbm, gather_ref), (offset_hbm, offset_ref))
        )
    ]
    scalars = [
        pltpu.make_async_copy(hbm, ref, sems.at[6 + a, 0])
        for a, (hbm, ref) in enumerate(((wave_hbm, wave_ref), (weight_hbm, weight_ref)))
    ]
    for copies in [scalars] + fetches:
        for copy in copies:
            copy.start()
    for copy in constants:
        copy.start()
    base = lax.axis_index("wave") * z.slots
    for copy in scalars:
        copy.wait()
    for j in range(z.rows):
        scale = weight_ref[j] * (1.0 / math.sqrt(z.lon))
        scale_ref[j * z.deep : (j + 1) * z.deep] = jnp.full((z.deep, lanes), scale, jnp.float32)
    height = 4 * z.levels
    degree = lax.broadcasted_iota(jnp.int32, (z.lats, z.degrees), 1)
    channel = lax.broadcasted_iota(jnp.int32, (height, z.lats), 0) // z.levels
    sign_sum = jnp.where(channel % 2 == 0, -1.0, 1.0)
    sign_slope = jnp.where(channel < 2, -1.0, 1.0)
    winds = []
    for (first, last), copies in zip(groups, fetches):
        waves = [wave_ref[base + s] for s in range(first, last)]
        for copy in copies:
            copy.wait()
        right = []
        for s, wave in zip(range(first, last), waves):
            live = jnp.where(degree >= wave, 1.0, 0.0).astype(jnp.bfloat16)
            masked = legendre_ref[s] * live
            live_ref[s] = masked
            right += [masked, derivative_ref[s] * live]
        left = [spectra_ref[s].reshape(height, z.degrees) for s in range(first, last)]
        sums = contract(jnp.concatenate(left, axis=0), jnp.concatenate(right, axis=0), ((1,), (1,)))
        for at, wave in enumerate(waves):
            mine = sums[at * height : (at + 1) * height]
            sums_at = mine[:, 2 * at * z.lats : (2 * at + 1) * z.lats]
            slopes = mine[:, (2 * at + 1) * z.lats : (2 * at + 2) * z.lats]
            turned = jnp.concatenate(
                [sums_at[c * z.levels : (c + 1) * z.levels] for c in (3, 2, 1, 0)], axis=0
            )
            scaled = wave.astype(jnp.float32) / z.degrees
            doubled = jnp.where(wave == 0, 1.0, 2.0)
            winds.append((scaled * sign_sum * turned + sign_slope * slopes) * doubled)
    winds = jnp.concatenate(winds, axis=0).astype(jnp.bfloat16)
    for copy in constants:
        copy.wait()

    def one_band(b, carry):
        choose = jnp.where(offset_ref[...] + b * z.rows == 0, 1.0, 0.0).astype(jnp.bfloat16)
        spread = contract(winds, choose, ((1,), (0,))) * pick_ref[...]
        piece = contract(gather_ref[...], spread.astype(jnp.bfloat16), ((1,), (0,)))
        piece = piece.astype(jnp.bfloat16)
        for l in range(z.sets):
            pieces_ref[b * z.sets + l] = piece
        return carry

    if z.bands <= 16:
        for b in range(z.bands):
            one_band(b, 0)
    else:
        lax.fori_loop(0, z.bands, one_band, 0)


def table_kernel(z, wave_ref, table_ref):
    wave = wave_ref[...].astype(jnp.float32)
    height = wave.shape[0]
    chunks = z.lon // lanes
    at = lax.broadcasted_iota(jnp.int32, (height, lanes), 1).astype(jnp.float32)

    def parts(phase):
        phase = phase - jnp.floor(phase * (1.0 / z.lon) + 0.5) * z.lon
        angle = phase * (2.0 * math.pi / z.lon)
        return jnp.cos(angle), jnp.sin(angle)

    fine_cos, fine_sin = parts(wave * at)
    coarse = [parts(wave * ((at + b) * lanes)) for b in range(0, chunks, lanes)]
    for a in range(chunks):
        cos_a = coarse[a // lanes][0][:, a % lanes : a % lanes + 1]
        sin_a = coarse[a // lanes][1][:, a % lanes : a % lanes + 1]
        columns = slice(a * lanes, (a + 1) * lanes)
        table_ref[:height, columns] = (cos_a * fine_cos - sin_a * fine_sin).astype(jnp.bfloat16)
        table_ref[height:, columns] = (-(sin_a * fine_cos + cos_a * fine_sin)).astype(jnp.bfloat16)


def by_parity(axis, first, second):
    even = lax.axis_index(axis) % 2 == 0
    return jnp.where(even, second, first), jnp.where(even, first, second)


def edge_kernel(z, own_ref, first_ref, second_ref, up_ref, down_ref):
    south, _ = by_parity("wave", first_ref[z.rows - 1], second_ref[z.rows - 1])
    _, north = by_parity("wave", first_ref[0], second_ref[0])
    even = lax.axis_index("lev") % 2 == 0
    rows = [south] + [own_ref[j] for j in range(z.rows)] + [north]
    plan = [(row, z.levels - 1, 0) for row in rows]
    plan += [(row, z.levels - 2, 1) for row in rows[1:-1]]
    plan += [(own_ref[z.rows + j], z.levels - 1, 0) for j in range(z.rows)]
    for at, (row, top, bottom) in enumerate(plan):
        top, bottom = row[top : top + 1], row[bottom : bottom + 1]
        up_ref[at : at + 1] = jnp.where(even, top, bottom)
        down_ref[at : at + 1] = jnp.where(even, bottom, top)


def grid_kernel(
    z,
    arrived_ref,
    unpack_ref,
    table_ref,
    own_ref,
    first_ref,
    second_ref,
    lev_first_ref,
    lev_second_ref,
    spread_ref,
    pick_ref,
    scale_ref,
    reply_ref,
    q_ref,
    f_ref,
):
    band, level_set = lax.axis_index("wave"), lax.axis_index("lev")
    lat_total = z.bands * z.rows
    lev_total = z.sets * z.levels
    own = slice(halo, halo + z.levels)
    q_ref[...] = jnp.zeros_like(q_ref)
    f_ref[...] = jnp.zeros_like(f_ref)
    for j in range(halo):
        south, north = by_parity("wave", first_ref[j], second_ref[j])
        q_ref[j, own] = south
        q_ref[halo + z.rows + j, own] = north
    south, north = by_parity("wave", first_ref[z.rows], second_ref[z.rows])
    f_ref[0, own] = south
    f_ref[z.rows + 1, own] = north
    for j in range(z.rows):
        q_ref[halo + j, own] = own_ref[j]
        f_ref[1 + j, own] = own_ref[z.rows + j]
    below, above = by_parity("lev", lev_first_ref[...], lev_second_ref[...])
    for got, near, far in ((below, halo - 1, 0), (above, halo + z.levels, z.deep - 1)):
        for j in range(z.rows + 2):
            q_ref[halo - 1 + j, near : near + 1] = got[j : j + 1]
        for j in range(z.rows):
            at = z.rows + 2 + j
            q_ref[halo + j, far : far + 1] = got[at : at + 1]
            at = 2 * z.rows + 2 + j
            f_ref[1 + j, near : near + 1] = got[at : at + 1]

    height = z.bands * z.slot_pad

    def from_set(index):
        return arrived_ref[:, index].reshape(height, z.piece)

    blocks = jnp.concatenate(
        [
            from_set(level_set),
            from_set(jnp.maximum(level_set - 1, 0)),
            from_set(jnp.minimum(level_set + 1, z.sets - 1)),
        ],
        axis=1,
    )
    turned = contract(unpack_ref[...], blocks, ((1,), (1,))).astype(jnp.bfloat16)
    span = turned.shape[0] // 2
    turned = jnp.concatenate([turned[:span], turned[span:]], axis=1)
    winds = contract(turned, table_ref[...], ((1,), (0,)))

    def wind(which, j):
        first = which * z.stack + j * z.deep
        return courant_limit * jnp.tanh(winds[first : first + z.deep])

    zonal = [wind(0, j) for j in range(1, z.rows + 3)]
    merid = [wind(1, j) for j in range(z.window)]

    def west(x):
        return pltpu.roll(x, 1, 1)

    def east(x):
        return pltpu.roll(x, z.lon - 1, 1)

    face = []
    for j in range(z.rows + 2):
        speed = 0.5 * (west(zonal[j]) + zonal[j])
        magnitude = jnp.abs(speed)
        diffuse = 0.5 * (magnitude - f_ref[j] * (magnitude - speed * speed))
        face.append((speed, diffuse))
    lat_face = []
    for j in range(1, z.window):
        index = band * z.rows - halo + j
        is_open = jnp.where((index > 0) & (index < lat_total), 0.5, 0.0).astype(jnp.float32)
        speed = 0.5 * (merid[j - 1] + merid[j])
        lat_face.append((speed * is_open, jnp.abs(speed) * is_open))
    deep = lax.broadcasted_iota(jnp.int32, (z.deep, z.lon), 0) + (level_set * z.levels - halo)
    rise = jnp.where((deep > 0) & (deep < lev_total), diffusivity, 0.0).astype(jnp.float32)

    def tendency(q, first):
        north_flux = []
        for j in range(len(q) - 1):
            mean, spread = lat_face[first - 1 + j]
            north_flux.append(mean * (q[j] + q[j + 1]) - spread * (q[j + 1] - q[j]))
        result = []
        for j in range(1, len(q) - 1):
            speed, diffuse = face[first - 2 + j]
            centre = q[j]
            western = west(centre)
            flux = speed * 0.5 * (western + centre) - diffuse * (centre - western)
            lift = rise * (centre - pltpu.roll(centre, 1, 0))
            result.append(
                -(east(flux) - flux)
                - (north_flux[j] - north_flux[j - 1])
                + (pltpu.roll(lift, z.deep - 1, 0) - lift)
            )
        return result

    tracer = [q_ref[j] for j in range(z.window)]
    first_tendency = tendency(tracer, 1)
    section_one = [q + t for q, t in zip(tracer[1:-1], first_tendency)]
    section_two = tendency(section_one, 2)
    tops, lows = [], []
    for j in range(z.rows):
        q = tracer[halo + j]
        change = 0.5 * q + 0.5 * (section_one[1 + j] + section_two[j]) - q
        top = change.astype(jnp.bfloat16)
        tops.append(top.astype(jnp.float32))
        lows.append(change - tops[-1])
    both = jnp.concatenate(tops + lows, axis=0).astype(jnp.bfloat16)
    projected = contract(both, table_ref[...], ((1,), (1,)))
    count = z.rows * z.deep
    projected = projected[:count] + projected[count:]
    scaled = projected * scale_ref[:, :1]
    top = scaled.astype(jnp.bfloat16)
    low = (scaled - top.astype(jnp.float32)).astype(jnp.bfloat16)
    both = jnp.concatenate([top, low], axis=0)
    for b in range(z.bands):
        first = b * z.slot_pad
        block = jnp.concatenate(
            [both[:, p * height + first : p * height + first + z.slot_pad] for p in range(2)], axis=1
        )
        block = contract(block, spread_ref[...], ((1,), (0,)))
        block = block[:count] + block[count:]
        for j in range(z.rows):
            mine = block[j * z.deep : (j + 1) * z.deep] * pick_ref[...]
            reply_ref[b, j : j + 1] = jnp.sum(mine, axis=0, keepdims=True)


def analysis_kernel(z, arrived_ref, live_ref, out_ref, turned_ref):
    arrived = arrived_ref[...].reshape(z.lats, z.reply)
    top = arrived.astype(jnp.bfloat16).astype(jnp.float32)
    turned = jnp.concatenate([top, arrived - top], axis=0)
    width = turned_ref.shape[2]
    for c in range(turned_ref.shape[0]):
        turned_ref[c] = turned[c * width : (c + 1) * width].T
    height = 2 * z.levels
    for s in range(z.slots):
        left = [
            turned_ref[c, pl.ds(s, height, stride=z.slot_pad), :].astype(jnp.bfloat16)
            for c in range(turned_ref.shape[0])
        ]
        left = jnp.concatenate(left, axis=1)
        right = jnp.concatenate([live_ref[s], live_ref[s]], axis=0)
        out_ref[s] = contract(left, right, ((1,), (0,))).reshape(2, z.levels, z.degrees)


def in_hbm(array):
    return pltpu.with_memory_space_constraint(array, pltpu.HBM)


def nbytes(array, dtype=None):
    return array.size * jnp.dtype(dtype or array.dtype).itemsize


def swaps(axis):
    count = lax.axis_size(axis)
    pairs = [[(i, i + 1) for i in range(start, count - 1, 2)] for start in (0, 1)]
    return [p + [(b, a) for a, b in p] for p in pairs]


def on_device(spectra, legendre, derivative, tracer, limiter_flags, lat_weight, slot_wave):
    z = Sizes(spectra, legendre, tracer, lax.axis_size("wave"), lax.axis_size("lev"))
    f32, bf16 = jnp.float32, jnp.bfloat16
    fan = 4 * z.bands * z.sets * z.slot_pad * z.piece
    table_bytes = 4 * z.bands * z.slot_pad * z.lon
    any_spec = pl.BlockSpec(memory_space=pltpu.HBM)
    edge_shape = jax.ShapeDtypeStruct((z.rows + 1, z.levels, z.lon), f32)
    own, to_first, to_second = pl.pallas_call(
        functools.partial(pack_kernel, z),
        name="pack",
        in_specs=[any_spec] * 2,
        out_specs=tuple(vmem(3)),
        out_shape=(
            jax.ShapeDtypeStruct((2 * z.rows, z.levels, z.lon), f32),
            edge_shape,
            edge_shape,
        ),
        scratch_shapes=[
            pltpu.VMEM(tracer.shape, tracer.dtype),
            pltpu.VMEM(tracer.shape, limiter_flags.dtype),
            pltpu.SemaphoreType.DMA((2,)),
        ],
        compiler_params=params(8 * nbytes(tracer)),
    )(in_hbm(tracer), in_hbm(limiter_flags))
    first_pairs, second_pairs = swaps("wave")
    wave_first = lax.ppermute(to_first, "wave", first_pairs)
    wave_second = lax.ppermute(to_second, "wave", second_pairs)
    constants = pack_constants(z)
    group_count = -(-z.slots // group_slots)
    pieces, live, scale = pl.pallas_call(
        functools.partial(legendre_kernel, z),
        name="legendre",
        in_specs=[any_spec] * 8,
        out_specs=tuple(vmem(3)),
        out_shape=(
            jax.ShapeDtypeStruct((z.bands * z.sets, z.slot_pad, z.piece), bf16),
            jax.ShapeDtypeStruct(legendre.shape, bf16),
            jax.ShapeDtypeStruct((z.rows * z.deep, lanes), f32),
        ),
        scratch_shapes=[pltpu.SMEM(x.shape, x.dtype) for x in (slot_wave, lat_weight)]
        + [pltpu.VMEM(x.shape, x.dtype) for x in (spectra, legendre, derivative, *constants)]
        + [pltpu.SemaphoreType.DMA((8, group_count))],
        compiler_params=params(2 * nbytes(spectra), 4 * nbytes(legendre), fan),
    )(*map(in_hbm, (slot_wave, lat_weight, spectra, legendre, derivative, *constants)))
    arrived = lax.all_to_all(pieces, ("wave", "lev"), split_axis=0, concat_axis=0, tiled=True)
    padded_wave = jnp.pad(
        slot_wave.reshape(z.bands, z.slots), ((0, 0), (0, z.slot_pad - z.slots))
    ).reshape(-1, 1)
    table = pl.pallas_call(
        functools.partial(table_kernel, z),
        name="table",
        in_specs=vmem(1),
        out_specs=vmem(1)[0],
        out_shape=jax.ShapeDtypeStruct((2 * z.bands * z.slot_pad, z.lon), bf16),
        compiler_params=params(table_bytes),
    )(padded_wave)
    up_shape = jax.ShapeDtypeStruct((3 * z.rows + 2, z.lon), f32)
    up, down = pl.pallas_call(
        functools.partial(edge_kernel, z),
        name="edges",
        in_specs=vmem(3),
        out_specs=tuple(vmem(2)),
        out_shape=(up_shape, up_shape),
        compiler_params=params(8 * nbytes(tracer)),
    )(own, wave_first, wave_second)
    first_pairs, second_pairs = swaps("lev")
    lev_first = lax.ppermute(up, "lev", first_pairs)
    lev_second = lax.ppermute(down, "lev", second_pairs)
    reply = pl.pallas_call(
        functools.partial(grid_kernel, z),
        name="grid",
        in_specs=vmem(11),
        out_specs=vmem(1)[0],
        out_shape=jax.ShapeDtypeStruct((z.bands, z.rows, z.reply), f32),
        scratch_shapes=[
            pltpu.VMEM((z.window, z.deep, z.lon), f32),
            pltpu.VMEM((z.rows + 2, z.deep, z.lon), f32),
        ],
        compiler_params=params(3 * table_bytes, 24 * nbytes(tracer), fan),
    )(
        arrived.reshape(z.bands, z.sets, z.slot_pad, z.piece),
        unpack_constant(z),
        table,
        own,
        wave_first,
        wave_second,
        lev_first,
        lev_second,
        *reply_constants(z),
        scale,
    )
    returned = lax.all_to_all(reply, "wave", split_axis=0, concat_axis=0, tiled=True)
    width = math.gcd(2 * z.lats, lanes)
    return pl.pallas_call(
        functools.partial(analysis_kernel, z),
        name="analysis",
        in_specs=vmem(2),
        out_specs=vmem(1)[0],
        out_shape=jax.ShapeDtypeStruct((z.slots, 2, z.levels, z.degrees), f32),
        scratch_shapes=[pltpu.VMEM((2 * z.lats // width, z.reply, width), f32)],
        compiler_params=params(nbytes(spectra, f32), nbytes(legendre)),
    )(returned, live)


def solution(mesh):
    return jax.shard_map(
        on_device,
        mesh=mesh,
        in_specs=(
            P("wave", None, "lev", None),
            P("wave", None, None),
            P("wave", None, None),
            P("lev", "wave", None),
            P("lev", "wave", None),
            P("wave"),
            P(),
        ),
        out_specs=P("wave", None, "lev", None),
        check_vma=False,
    )
```

```python
import functools
import math

import jax
import jax.numpy as jnp
import numpy as np
from jax import lax
from jax.experimental import pallas as pl
from jax.experimental.pallas import tpu as pltpu
from jax.sharding import PartitionSpec as P

diffusivity = 0.15
courant_limit = 0.45
halo = 2
lanes = 128
packed_rows = 16


def round_up(value, step):
    return -(-value // step) * step


def contract(left, right, dims):
    return lax.dot_general(left, right, (dims, ((), ())), preferred_element_type=jnp.float32)


def vmem(count):
    return [pl.BlockSpec(memory_space=pltpu.VMEM)] * count


def params(*byte_counts):
    return pltpu.CompilerParams(vmem_limit_bytes=min(60 * 2**20, 6 * 2**20 + sum(byte_counts)))


class Sizes:
    def __init__(self, spectra, legendre, tracer, bands, sets):
        self.slots, _, self.levels, self.degrees = spectra.shape
        self.lats = legendre.shape[1]
        self.rows, self.lon = tracer.shape[1:]
        self.bands, self.sets = bands, sets
        self.slot_pad = round_up(self.slots, packed_rows)
        self.window = self.rows + 2 * halo
        self.deep = self.levels + 2 * halo
        self.unit = 4 * self.levels
        self.piece = round_up(self.window * self.unit, lanes)
        self.stack = round_up(self.window * self.deep, 8)
        self.reply = round_up(2 * self.levels * self.slot_pad, lanes)
        assert self.rows == halo and self.deep == 8 and self.lon % lanes == 0
        assert lanes % self.unit == 0 and self.lats % 8 == 0


def piece_lanes(z):
    at = np.arange(z.piece)
    row, channel, level = at // z.unit, at // z.levels % 4, at % z.levels
    return channel % 2, channel // 2, row, level, row < z.window


def unpack_constant(z):
    part, wind, row, level, valid = piece_lanes(z)
    height = round_up(2 * z.stack, lanes)
    target = np.arange(2 * height)
    t_part, rest = target // height, target % height
    t_wind, rest = rest // z.stack, rest % z.stack
    t_row, t_deep = rest // z.deep, rest % z.deep
    t_valid = (t_wind < 2) & (t_row < z.window)
    same = (t_part[:, None] == part) & (t_wind[:, None] == wind) & (t_row[:, None] == row)
    same = same & valid & t_valid[:, None]
    own = same & (t_deep[:, None] == level + halo)
    below = same & (t_deep[:, None] == halo - 1) & (level == z.levels - 1)
    above = same & (t_deep[:, None] == halo + z.levels) & (level == 0)
    return jnp.asarray(np.concatenate([own, below, above], axis=1), jnp.bfloat16)


def reply_constants(z):
    at = np.arange(z.reply)
    part, rest = at // (z.levels * z.slot_pad), at % (z.levels * z.slot_pad)
    level, slot = rest // z.slot_pad, rest % z.slot_pad
    source = np.arange(2 * z.slot_pad)
    spread = (source[:, None] // z.slot_pad == part) & (source[:, None] % z.slot_pad == slot)
    pick = np.arange(z.deep)[:, None] == level + halo
    return jnp.asarray(spread, jnp.bfloat16), pick.astype(np.float32)


def legendre_kernel(
    z,
    wave_hbm,
    weight_hbm,
    spectra_hbm,
    legendre_hbm,
    derivative_hbm,
    tracer_hbm,
    flags_hbm,
    pieces_ref,
    live_ref,
    scale_ref,
    own_ref,
    first_ref,
    second_ref,
    wave_ref,
    weight_ref,
    spectra_ref,
    legendre_ref,
    derivative_ref,
    tracer_ref,
    flags_ref,
    by_slot_ref,
    sems,
):
    group_slots = lanes // z.unit
    groups = [
        (first, min(first + group_slots, z.slots)) for first in range(0, z.slots, group_slots)
    ]
    whole = [
        pltpu.make_async_copy(hbm, ref, sems.at[a, 0])
        for a, (hbm, ref) in enumerate(
            (
                (wave_hbm, wave_ref),
                (weight_hbm, weight_ref),
                (tracer_hbm, tracer_ref),
                (flags_hbm, flags_ref),
            )
        )
    ]
    fetches = []
    for g, (first, last) in enumerate(groups):
        part = pl.ds(first, last - first)
        fetches.append(
            [
                pltpu.make_async_copy(hbm.at[part], ref.at[part], sems.at[4 + a, g])
                for a, (hbm, ref) in enumerate(
                    (
                        (legendre_hbm, legendre_ref),
                        (derivative_hbm, derivative_ref),
                        (spectra_hbm, spectra_ref),
                    )
                )
            ]
        )
    for copies in [whole[:2], *fetches, whole[2:]]:
        for copy in copies:
            copy.start()
    base = lax.axis_index("wave") * z.slots
    by_slot_ref[...] = jnp.zeros_like(by_slot_ref)
    whole[0].wait()
    whole[1].wait()
    for j in range(z.rows):
        scale = weight_ref[j] * (1.0 / math.sqrt(z.lon))
        scale_ref[j * z.deep : (j + 1) * z.deep] = jnp.full((z.deep, lanes), scale, jnp.float32)
    degree = lax.broadcasted_iota(jnp.int32, (z.lats, z.degrees), 1)
    lane = lax.broadcasted_iota(jnp.int32, (z.lats, lanes), 1)
    lane_slot, channel = lane // z.unit, lane // z.levels % 4
    sign_sum = jnp.where(channel % 2 == 0, -1.0, 1.0)
    sign_slope = jnp.where(channel < 2, -1.0, 1.0)
    for (first, last), copies in zip(groups, fetches):
        waves = [wave_ref[base + s] for s in range(first, last)]
        for copy in copies:
            copy.wait()
        sums, slopes = [], []
        for s, wave in zip(range(first, last), waves):
            live = jnp.where(degree >= wave, 1.0, 0.0).astype(jnp.bfloat16)
            masked = legendre_ref[s] * live
            live_ref[s] = masked
            sums.append(masked)
            slopes.append(derivative_ref[s] * live)
        right = [spectra_ref[s].reshape(z.unit, z.degrees) for s in range(first, last)]
        right += [jnp.zeros_like(right[0])] * (group_slots - len(right))
        right = jnp.concatenate(right, axis=0)
        sums = contract(jnp.concatenate(sums, axis=0), right, ((1,), (1,)))
        slopes = contract(jnp.concatenate(slopes, axis=0), right, ((1,), (1,)))
        sum_of = jnp.zeros((z.lats, lanes), jnp.float32)
        slope_of = sum_of
        factor = sum_of
        doubled = sum_of
        for at, wave in enumerate(waves):
            mine = lane_slot == at
            block = slice(at * z.lats, (at + 1) * z.lats)
            sum_of = jnp.where(mine, sums[block], sum_of)
            slope_of = jnp.where(mine, slopes[block], slope_of)
            factor = jnp.where(mine, wave.astype(jnp.float32) / z.degrees, factor)
            doubled = jnp.where(mine, jnp.where(wave == 0, 1.0, 2.0), doubled)
        turned = sum_of
        for c in range(4):
            moved = pltpu.roll(sum_of, (2 * c - 3) * z.levels % lanes, 1)
            turned = jnp.where(channel == c, moved, turned)
        winds = (factor * sign_sum * turned + sign_slope * slope_of) * doubled
        for at, s in enumerate(range(first, last)):
            moved = winds if at == 0 else pltpu.roll(winds, lanes - at * z.unit, 1)
            by_slot_ref[s * z.lats : (s + 1) * z.lats] = moved
    tiles = round_up((z.lats + 2 * halo) * z.unit, lanes) // lanes + z.piece // lanes
    rows = [jnp.zeros((z.slot_pad, lanes), jnp.float32) for _ in range(tiles)]
    slot_lane = lax.broadcasted_iota(jnp.int32, (z.slot_pad, lanes), 1) // z.unit
    for lat in range(z.lats):
        tile, at = divmod((lat + halo) * z.unit, lanes)
        block = by_slot_ref[pl.ds(lat, z.slot_pad, stride=z.lats), :]
        block = block if at == 0 else pltpu.roll(block, at, 1)
        rows[tile] = jnp.where(slot_lane == at // z.unit, block, rows[tile])
    rows = jnp.concatenate(rows, axis=1)
    for b in range(z.bands):
        at = b * z.rows * z.unit
        piece = rows[:, at : at + z.piece].astype(jnp.bfloat16)
        for l in range(z.sets):
            pieces_ref[b * z.sets + l] = piece

    even = lax.axis_index("wave") % 2 == 0
    whole[2].wait()
    for j in range(z.rows):
        row = tracer_ref[:, j, :]
        own_ref[j] = row
        first_ref[j] = row
        second_ref[j] = row
    whole[3].wait()
    switched = [flags_ref[:, j, :].astype(jnp.float32) for j in range(z.rows)]
    for j in range(z.rows):
        own_ref[z.rows + j] = switched[j]
    first_ref[z.rows] = jnp.where(even, switched[-1], switched[0])
    second_ref[z.rows] = jnp.where(even, switched[0], switched[-1])


def table_kernel(z, wave_ref, table_ref):
    wave = wave_ref[...].astype(jnp.float32)
    height = wave.shape[0]
    chunks = z.lon // lanes
    at = lax.broadcasted_iota(jnp.int32, (height, lanes), 1).astype(jnp.float32)

    def parts(phase):
        phase = phase - jnp.floor(phase * (1.0 / z.lon) + 0.5) * z.lon
        angle = phase * (2.0 * math.pi / z.lon)
        return jnp.cos(angle), jnp.sin(angle)

    fine_cos, fine_sin = parts(wave * at)
    coarse = [parts(wave * ((at + b) * lanes)) for b in range(0, chunks, lanes)]
    for a in range(chunks):
        cos_a = coarse[a // lanes][0][:, a % lanes : a % lanes + 1]
        sin_a = coarse[a // lanes][1][:, a % lanes : a % lanes + 1]
        columns = slice(a * lanes, (a + 1) * lanes)
        table_ref[:height, columns] = (cos_a * fine_cos - sin_a * fine_sin).astype(jnp.bfloat16)
        table_ref[height:, columns] = (-(sin_a * fine_cos + cos_a * fine_sin)).astype(jnp.bfloat16)


def by_parity(axis, first, second):
    even = lax.axis_index(axis) % 2 == 0
    return jnp.where(even, second, first), jnp.where(even, first, second)


def edge_kernel(z, own_ref, first_ref, second_ref, up_ref, down_ref):
    south, _ = by_parity("wave", first_ref[z.rows - 1], second_ref[z.rows - 1])
    _, north = by_parity("wave", first_ref[0], second_ref[0])
    even = lax.axis_index("lev") % 2 == 0
    rows = [south] + [own_ref[j] for j in range(z.rows)] + [north]
    plan = [(row, z.levels - 1, 0) for row in rows]
    plan += [(row, z.levels - 2, 1) for row in rows[1:-1]]
    plan += [(own_ref[z.rows + j], z.levels - 1, 0) for j in range(z.rows)]
    for at, (row, top, bottom) in enumerate(plan):
        top, bottom = row[top : top + 1], row[bottom : bottom + 1]
        up_ref[at : at + 1] = jnp.where(even, top, bottom)
        down_ref[at : at + 1] = jnp.where(even, bottom, top)


def grid_kernel(
    z,
    arrived_ref,
    unpack_ref,
    table_ref,
    own_ref,
    first_ref,
    second_ref,
    lev_first_ref,
    lev_second_ref,
    spread_ref,
    pick_ref,
    scale_ref,
    reply_ref,
    q_ref,
    f_ref,
):
    band, level_set = lax.axis_index("wave"), lax.axis_index("lev")
    lat_total = z.bands * z.rows
    lev_total = z.sets * z.levels
    own = slice(halo, halo + z.levels)
    q_ref[...] = jnp.zeros_like(q_ref)
    f_ref[...] = jnp.zeros_like(f_ref)
    for j in range(halo):
        south, north = by_parity("wave", first_ref[j], second_ref[j])
        q_ref[j, own] = south
        q_ref[halo + z.rows + j, own] = north
    south, north = by_parity("wave", first_ref[z.rows], second_ref[z.rows])
    f_ref[0, own] = south
    f_ref[z.rows + 1, own] = north
    for j in range(z.rows):
        q_ref[halo + j, own] = own_ref[j]
        f_ref[1 + j, own] = own_ref[z.rows + j]
    below, above = by_parity("lev", lev_first_ref[...], lev_second_ref[...])
    for got, near, far in ((below, halo - 1, 0), (above, halo + z.levels, z.deep - 1)):
        for j in range(z.rows + 2):
            q_ref[halo - 1 + j, near : near + 1] = got[j : j + 1]
        for j in range(z.rows):
            at = z.rows + 2 + j
            q_ref[halo + j, far : far + 1] = got[at : at + 1]
            at = 2 * z.rows + 2 + j
            f_ref[1 + j, near : near + 1] = got[at : at + 1]

    height = z.bands * z.slot_pad

    def from_set(index):
        return arrived_ref[:, index].reshape(height, z.piece)

    blocks = jnp.concatenate(
        [
            from_set(level_set),
            from_set(jnp.maximum(level_set - 1, 0)),
            from_set(jnp.minimum(level_set + 1, z.sets - 1)),
        ],
        axis=1,
    )
    turned = contract(unpack_ref[...], blocks, ((1,), (1,))).astype(jnp.bfloat16)
    span = turned.shape[0] // 2
    turned = jnp.concatenate([turned[:span], turned[span:]], axis=1)
    winds = contract(turned, table_ref[...], ((1,), (0,)))

    def wind(which, j):
        first = which * z.stack + j * z.deep
        return courant_limit * jnp.tanh(winds[first : first + z.deep])

    zonal = [wind(0, j) for j in range(1, z.rows + 3)]
    merid = [wind(1, j) for j in range(z.window)]

    def west(x):
        return pltpu.roll(x, 1, 1)

    def east(x):
        return pltpu.roll(x, z.lon - 1, 1)

    face = []
    for j in range(z.rows + 2):
        speed = 0.5 * (west(zonal[j]) + zonal[j])
        magnitude = jnp.abs(speed)
        diffuse = 0.5 * (magnitude - f_ref[j] * (magnitude - speed * speed))
        face.append((speed, diffuse))
    lat_face = []
    for j in range(1, z.window):
        index = band * z.rows - halo + j
        is_open = jnp.where((index > 0) & (index < lat_total), 0.5, 0.0).astype(jnp.float32)
        speed = 0.5 * (merid[j - 1] + merid[j])
        lat_face.append((speed * is_open, jnp.abs(speed) * is_open))
    deep = lax.broadcasted_iota(jnp.int32, (z.deep, z.lon), 0) + (level_set * z.levels - halo)
    rise = jnp.where((deep > 0) & (deep < lev_total), diffusivity, 0.0).astype(jnp.float32)

    def tendency(q, first):
        north_flux = []
        for j in range(len(q) - 1):
            mean, spread = lat_face[first - 1 + j]
            north_flux.append(mean * (q[j] + q[j + 1]) - spread * (q[j + 1] - q[j]))
        result = []
        for j in range(1, len(q) - 1):
            speed, diffuse = face[first - 2 + j]
            centre = q[j]
            western = west(centre)
            flux = speed * 0.5 * (western + centre) - diffuse * (centre - western)
            lift = rise * (centre - pltpu.roll(centre, 1, 0))
            result.append(
                -(east(flux) - flux)
                - (north_flux[j] - north_flux[j - 1])
                + (pltpu.roll(lift, z.deep - 1, 0) - lift)
            )
        return result

    tracer = [q_ref[j] for j in range(z.window)]
    first_tendency = tendency(tracer, 1)
    section_one = [q + t for q, t in zip(tracer[1:-1], first_tendency)]
    section_two = tendency(section_one, 2)
    tops, lows = [], []
    for j in range(z.rows):
        q = tracer[halo + j]
        change = 0.5 * q + 0.5 * (section_one[1 + j] + section_two[j]) - q
        top = change.astype(jnp.bfloat16)
        tops.append(top.astype(jnp.float32))
        lows.append(change - tops[-1])
    both = jnp.concatenate(tops + lows, axis=0).astype(jnp.bfloat16)
    projected = contract(both, table_ref[...], ((1,), (1,)))
    count = z.rows * z.deep
    projected = projected[:count] + projected[count:]
    scaled = projected * scale_ref[:, :1]
    top = scaled.astype(jnp.bfloat16)
    low = (scaled - top.astype(jnp.float32)).astype(jnp.bfloat16)
    both = jnp.concatenate([top, low], axis=0)
    for b in range(z.bands):
        first = b * z.slot_pad
        block = jnp.concatenate(
            [both[:, p * height + first : p * height + first + z.slot_pad] for p in range(2)], axis=1
        )
        block = contract(block, spread_ref[...], ((1,), (0,)))
        block = block[:count] + block[count:]
        for j in range(z.rows):
            mine = block[j * z.deep : (j + 1) * z.deep] * pick_ref[...]
            reply_ref[b, j : j + 1] = jnp.sum(mine, axis=0, keepdims=True)


def analysis_kernel(z, arrived_ref, live_ref, out_ref, turned_ref):
    arrived = arrived_ref[...].reshape(z.lats, z.reply)
    top = arrived.astype(jnp.bfloat16).astype(jnp.float32)
    turned = jnp.concatenate([top, arrived - top], axis=0)
    width = turned_ref.shape[2]
    for c in range(turned_ref.shape[0]):
        turned_ref[c] = turned[c * width : (c + 1) * width].T
    height = 2 * z.levels
    for s in range(z.slots):
        left = [
            turned_ref[c, pl.ds(s, height, stride=z.slot_pad), :].astype(jnp.bfloat16)
            for c in range(turned_ref.shape[0])
        ]
        left = jnp.concatenate(left, axis=1)
        right = jnp.concatenate([live_ref[s], live_ref[s]], axis=0)
        out_ref[s] = contract(left, right, ((1,), (0,))).reshape(2, z.levels, z.degrees)


def in_hbm(array):
    return pltpu.with_memory_space_constraint(array, pltpu.HBM)


def nbytes(array, dtype=None):
    return array.size * jnp.dtype(dtype or array.dtype).itemsize


def swaps(axis):
    count = lax.axis_size(axis)
    pairs = [[(i, i + 1) for i in range(start, count - 1, 2)] for start in (0, 1)]
    return [p + [(b, a) for a, b in p] for p in pairs]


def on_device(spectra, legendre, derivative, tracer, limiter_flags, lat_weight, slot_wave):
    z = Sizes(spectra, legendre, tracer, lax.axis_size("wave"), lax.axis_size("lev"))
    f32, bf16 = jnp.float32, jnp.bfloat16
    fan = 4 * z.bands * z.sets * z.slot_pad * z.piece
    table_bytes = 4 * z.bands * z.slot_pad * z.lon
    any_spec = pl.BlockSpec(memory_space=pltpu.HBM)
    edge_shape = jax.ShapeDtypeStruct((z.rows + 1, z.levels, z.lon), f32)
    group_count = -(-z.slots * z.unit // lanes)
    fetched = (slot_wave, lat_weight, spectra, legendre, derivative, tracer, limiter_flags)
    pieces, live, scale, own, to_first, to_second = pl.pallas_call(
        functools.partial(legendre_kernel, z),
        name="legendre",
        in_specs=[any_spec] * len(fetched),
        out_specs=tuple(vmem(6)),
        out_shape=(
            jax.ShapeDtypeStruct((z.bands * z.sets, z.slot_pad, z.piece), bf16),
            jax.ShapeDtypeStruct(legendre.shape, bf16),
            jax.ShapeDtypeStruct((z.rows * z.deep, lanes), f32),
            jax.ShapeDtypeStruct((2 * z.rows, z.levels, z.lon), f32),
            edge_shape,
            edge_shape,
        ),
        scratch_shapes=[pltpu.SMEM(x.shape, x.dtype) for x in fetched[:2]]
        + [pltpu.VMEM(x.shape, x.dtype) for x in fetched[2:]]
        + [
            pltpu.VMEM((z.slot_pad * z.lats, lanes), f32),
            pltpu.SemaphoreType.DMA((7, group_count)),
        ],
        compiler_params=params(
            2 * nbytes(spectra), 6 * nbytes(legendre), 8 * nbytes(tracer), fan
        ),
    )(*map(in_hbm, fetched))
    first_pairs, second_pairs = swaps("wave")
    wave_first = lax.ppermute(to_first, "wave", first_pairs)
    wave_second = lax.ppermute(to_second, "wave", second_pairs)
    arrived = lax.all_to_all(pieces, ("wave", "lev"), split_axis=0, concat_axis=0, tiled=True)
    padded_wave = jnp.pad(
        slot_wave.reshape(z.bands, z.slots), ((0, 0), (0, z.slot_pad - z.slots))
    ).reshape(-1, 1)
    table = pl.pallas_call(
        functools.partial(table_kernel, z),
        name="table",
        in_specs=vmem(1),
        out_specs=vmem(1)[0],
        out_shape=jax.ShapeDtypeStruct((2 * z.bands * z.slot_pad, z.lon), bf16),
        compiler_params=params(table_bytes),
    )(padded_wave)
    up_shape = jax.ShapeDtypeStruct((3 * z.rows + 2, z.lon), f32)
    up, down = pl.pallas_call(
        functools.partial(edge_kernel, z),
        name="edges",
        in_specs=vmem(3),
        out_specs=tuple(vmem(2)),
        out_shape=(up_shape, up_shape),
        compiler_params=params(8 * nbytes(tracer)),
    )(own, wave_first, wave_second)
    first_pairs, second_pairs = swaps("lev")
    lev_first = lax.ppermute(up, "lev", first_pairs)
    lev_second = lax.ppermute(down, "lev", second_pairs)
    reply = pl.pallas_call(
        functools.partial(grid_kernel, z),
        name="grid",
        in_specs=vmem(11),
        out_specs=vmem(1)[0],
        out_shape=jax.ShapeDtypeStruct((z.bands, z.rows, z.reply), f32),
        scratch_shapes=[
            pltpu.VMEM((z.window, z.deep, z.lon), f32),
            pltpu.VMEM((z.rows + 2, z.deep, z.lon), f32),
        ],
        compiler_params=params(3 * table_bytes, 24 * nbytes(tracer), fan),
    )(
        arrived.reshape(z.bands, z.sets, z.slot_pad, z.piece),
        unpack_constant(z),
        table,
        own,
        wave_first,
        wave_second,
        lev_first,
        lev_second,
        *reply_constants(z),
        scale,
    )
    returned = lax.all_to_all(reply, "wave", split_axis=0, concat_axis=0, tiled=True)
    width = math.gcd(2 * z.lats, lanes)
    return pl.pallas_call(
        functools.partial(analysis_kernel, z),
        name="analysis",
        in_specs=vmem(2),
        out_specs=vmem(1)[0],
        out_shape=jax.ShapeDtypeStruct((z.slots, 2, z.levels, z.degrees), f32),
        scratch_shapes=[pltpu.VMEM((2 * z.lats // width, z.reply, width), f32)],
        compiler_params=params(nbytes(spectra, f32), nbytes(legendre)),
    )(returned, live)


def solution(mesh):
    return jax.shard_map(
        on_device,
        mesh=mesh,
        in_specs=(
            P("wave", None, "lev", None),
            P("wave", None, None),
            P("wave", None, None),
            P("lev", "wave", None),
            P("lev", "wave", None),
            P("wave"),
            P(),
        ),
        out_specs=P("wave", None, "lev", None),
        check_vma=False,
    )
```

```python
import functools
import math

import jax
import jax.numpy as jnp
import numpy as np
from jax import lax
from jax.experimental import pallas as pl
from jax.experimental.pallas import tpu as pltpu
from jax.sharding import PartitionSpec as P

diffusivity = 0.15
courant_limit = 0.45
halo = 2
lanes = 128
packed_rows = 16


def round_up(value, step):
    return -(-value // step) * step


def contract(left, right, dims):
    return lax.dot_general(left, right, (dims, ((), ())), preferred_element_type=jnp.float32)


def vmem(count):
    return [pl.BlockSpec(memory_space=pltpu.VMEM)] * count


def params(*byte_counts):
    return pltpu.CompilerParams(vmem_limit_bytes=min(60 * 2**20, 6 * 2**20 + sum(byte_counts)))


class Sizes:
    def __init__(self, spectra, legendre, tracer, bands, sets):
        self.slots, _, self.levels, self.degrees = spectra.shape
        self.lats = legendre.shape[1]
        self.rows, self.lon = tracer.shape[1:]
        self.bands, self.sets = bands, sets
        self.slot_pad = round_up(self.slots, packed_rows)
        self.window = self.rows + 2 * halo
        self.block = self.rows * self.levels
        self.unit = 4 * self.levels
        self.piece = round_up(self.window * self.unit, lanes)
        self.reply = round_up(2 * self.levels * self.slot_pad, lanes)
        assert self.rows == halo and self.block == 8 and self.lon % lanes == 0
        assert lanes % self.unit == 0 and self.lats % 8 == 0


def piece_lanes(z):
    at = np.arange(z.piece)
    row, channel, level = at // z.unit, at // z.levels % 4, at % z.levels
    return channel % 2, channel // 2, row, level, row < z.window


def unpack_constant(z):
    part, wind, row, level, valid = piece_lanes(z)
    tiles = [(0, 0, 1), (0, 2, -1), (1, -2, -1), (1, 0, 1), (1, 2, 3)]
    target = [
        (of, pair[j], k) for of, *pair in tiles for j in range(z.rows) for k in range(z.levels)
    ]
    target += [(-1, 0, 0)] * (round_up(len(target), packed_rows) - len(target))
    t_wind, t_row, t_level = (np.array(x)[:, None] for x in zip(*target))
    same = (t_wind == wind) & (t_row + halo == row) & (t_level == level) & valid
    both = np.concatenate([same & (part == 0), same & (part == 1)], axis=0)
    return jnp.asarray(both, jnp.bfloat16)


def reply_constants(z):
    at = np.arange(z.reply)
    part, rest = at // (z.levels * z.slot_pad), at % (z.levels * z.slot_pad)
    level, slot = rest // z.slot_pad, rest % z.slot_pad
    source = np.arange(2 * z.slot_pad)
    spread = (source[:, None] // z.slot_pad == part) & (source[:, None] % z.slot_pad == slot)
    k = np.arange(z.block)[:, None] % z.levels
    edge = 0.5 * diffusivity
    picks = [
        1.0 * (k == level),
        edge * ((k == z.levels - 1) & (level == 0)),
        edge * ((k == 0) & (level == z.levels - 1)),
    ]
    return jnp.asarray(spread, jnp.bfloat16), np.stack(picks).astype(np.float32)


def legendre_kernel(
    z,
    wave_hbm,
    weight_hbm,
    spectra_hbm,
    legendre_hbm,
    derivative_hbm,
    tracer_hbm,
    flags_hbm,
    pieces_ref,
    live_ref,
    scale_ref,
    own_ref,
    first_ref,
    second_ref,
    wave_ref,
    weight_ref,
    spectra_ref,
    legendre_ref,
    derivative_ref,
    tracer_ref,
    flags_ref,
    by_slot_ref,
    sems,
):
    group_slots = lanes // z.unit
    groups = [
        (first, min(first + group_slots, z.slots)) for first in range(0, z.slots, group_slots)
    ]
    whole = [
        pltpu.make_async_copy(hbm, ref, sems.at[a, 0])
        for a, (hbm, ref) in enumerate(
            (
                (wave_hbm, wave_ref),
                (weight_hbm, weight_ref),
                (tracer_hbm, tracer_ref),
                (flags_hbm, flags_ref),
            )
        )
    ]
    fetches = []
    for g, (first, last) in enumerate(groups):
        part = pl.ds(first, last - first)
        fetches.append(
            [
                pltpu.make_async_copy(hbm.at[part], ref.at[part], sems.at[4 + a, g])
                for a, (hbm, ref) in enumerate(
                    (
                        (legendre_hbm, legendre_ref),
                        (derivative_hbm, derivative_ref),
                        (spectra_hbm, spectra_ref),
                    )
                )
            ]
        )
    for copies in [whole[:2], *fetches, whole[2:]]:
        for copy in copies:
            copy.start()
    base = lax.axis_index("wave") * z.slots
    by_slot_ref[...] = jnp.zeros_like(by_slot_ref)
    whole[0].wait()
    whole[1].wait()
    for j in range(z.rows):
        scale = weight_ref[j] * (1.0 / math.sqrt(z.lon))
        block = slice(j * z.levels, (j + 1) * z.levels)
        scale_ref[block] = jnp.full((z.levels, lanes), scale, jnp.float32)
    degree = lax.broadcasted_iota(jnp.int32, (z.lats, z.degrees), 1)
    lane = lax.broadcasted_iota(jnp.int32, (z.lats, lanes), 1)
    lane_slot, channel = lane // z.unit, lane // z.levels % 4
    sign_sum = jnp.where(channel % 2 == 0, -1.0, 1.0)
    sign_slope = jnp.where(channel < 2, -1.0, 1.0)
    for (first, last), copies in zip(groups, fetches):
        waves = [wave_ref[base + s] for s in range(first, last)]
        for copy in copies:
            copy.wait()
        sums, slopes = [], []
        for s, wave in zip(range(first, last), waves):
            live = jnp.where(degree >= wave, 1.0, 0.0).astype(jnp.bfloat16)
            masked = legendre_ref[s] * live
            live_ref[s] = masked
            sums.append(masked)
            slopes.append(derivative_ref[s] * live)
        right = [spectra_ref[s].reshape(z.unit, z.degrees) for s in range(first, last)]
        right += [jnp.zeros_like(right[0])] * (group_slots - len(right))
        right = jnp.concatenate(right, axis=0)
        sums = contract(jnp.concatenate(sums, axis=0), right, ((1,), (1,)))
        slopes = contract(jnp.concatenate(slopes, axis=0), right, ((1,), (1,)))
        sum_of = jnp.zeros((z.lats, lanes), jnp.float32)
        slope_of = sum_of
        factor = sum_of
        doubled = sum_of
        for at, wave in enumerate(waves):
            mine = lane_slot == at
            block = slice(at * z.lats, (at + 1) * z.lats)
            sum_of = jnp.where(mine, sums[block], sum_of)
            slope_of = jnp.where(mine, slopes[block], slope_of)
            factor = jnp.where(mine, wave.astype(jnp.float32) / z.degrees, factor)
            doubled = jnp.where(mine, jnp.where(wave == 0, 1.0, 2.0), doubled)
        turned = sum_of
        for c in range(4):
            moved = pltpu.roll(sum_of, (2 * c - 3) * z.levels % lanes, 1)
            turned = jnp.where(channel == c, moved, turned)
        winds = (factor * sign_sum * turned + sign_slope * slope_of) * doubled
        for at, s in enumerate(range(first, last)):
            moved = winds if at == 0 else pltpu.roll(winds, lanes - at * z.unit, 1)
            by_slot_ref[s * z.lats : (s + 1) * z.lats] = moved
    tiles = round_up((z.lats + 2 * halo) * z.unit, lanes) // lanes + z.piece // lanes
    rows = [jnp.zeros((z.slot_pad, lanes), jnp.float32) for _ in range(tiles)]
    slot_lane = lax.broadcasted_iota(jnp.int32, (z.slot_pad, lanes), 1) // z.unit
    for lat in range(z.lats):
        tile, at = divmod((lat + halo) * z.unit, lanes)
        block = by_slot_ref[pl.ds(lat, z.slot_pad, stride=z.lats), :]
        block = block if at == 0 else pltpu.roll(block, at, 1)
        rows[tile] = jnp.where(slot_lane == at // z.unit, block, rows[tile])
    rows = jnp.concatenate(rows, axis=1)
    for b in range(z.bands):
        at = b * z.rows * z.unit
        pieces_ref[b] = rows[:, at : at + z.piece].astype(jnp.bfloat16)

    even = lax.axis_index("wave") % 2 == 0
    whole[2].wait()
    for j in range(z.rows):
        row = tracer_ref[:, j, :]
        own_ref[j] = row
        first_ref[j] = row
        second_ref[j] = row
    whole[3].wait()
    switched = [flags_ref[:, j, :].astype(jnp.float32) for j in range(z.rows)]
    for j in range(z.rows):
        own_ref[z.rows + j] = switched[j]
    first_ref[z.rows] = jnp.where(even, switched[-1], switched[0])
    second_ref[z.rows] = jnp.where(even, switched[0], switched[-1])


def table_kernel(z, wave_ref, table_ref):
    wave = wave_ref[...].astype(jnp.float32)
    height = wave.shape[0]
    chunks = z.lon // lanes
    at = lax.broadcasted_iota(jnp.int32, (height, lanes), 1).astype(jnp.float32)

    def parts(phase):
        phase = phase - jnp.floor(phase * (1.0 / z.lon) + 0.5) * z.lon
        angle = phase * (2.0 * math.pi / z.lon)
        return jnp.cos(angle), jnp.sin(angle)

    fine_cos, fine_sin = parts(wave * at)
    coarse = [parts(wave * ((at + b) * lanes)) for b in range(0, chunks, lanes)]
    for a in range(chunks):
        cos_a = coarse[a // lanes][0][:, a % lanes : a % lanes + 1]
        sin_a = coarse[a // lanes][1][:, a % lanes : a % lanes + 1]
        columns = slice(a * lanes, (a + 1) * lanes)
        table_ref[:height, columns] = (cos_a * fine_cos - sin_a * fine_sin).astype(jnp.bfloat16)
        table_ref[height:, columns] = (-(sin_a * fine_cos + cos_a * fine_sin)).astype(jnp.bfloat16)


def by_parity(axis, first, second):
    even = lax.axis_index(axis) % 2 == 0
    return jnp.where(even, second, first), jnp.where(even, first, second)


def edge_kernel(z, own_ref, first_ref, second_ref, up_ref, down_ref):
    south, _ = by_parity("wave", first_ref[z.rows - 1], second_ref[z.rows - 1])
    _, north = by_parity("wave", first_ref[0], second_ref[0])
    even = lax.axis_index("lev") % 2 == 0
    rows = [south] + [own_ref[j] for j in range(z.rows)] + [north]
    for at, row in enumerate(rows):
        top, bottom = row[z.levels - 1 :], row[:1]
        up_ref[at : at + 1] = jnp.where(even, top, bottom)
        down_ref[at : at + 1] = jnp.where(even, bottom, top)


def grid_kernel(
    z,
    arrived_ref,
    unpack_ref,
    table_ref,
    own_ref,
    first_ref,
    second_ref,
    lev_first_ref,
    lev_second_ref,
    spread_ref,
    pick_ref,
    scale_ref,
    reply_ref,
):
    band, level_set = lax.axis_index("wave"), lax.axis_index("lev")
    lat_total = z.bands * z.rows
    lev_total = z.sets * z.levels
    height = z.bands * z.slot_pad
    f32 = jnp.float32

    turned = contract(unpack_ref[...], arrived_ref[...].reshape(height, z.piece), ((1,), (1,)))
    turned = turned.astype(jnp.bfloat16)
    span = turned.shape[0] // 2
    turned = jnp.concatenate([turned[:span], turned[span:]], axis=1)
    winds = contract(turned, table_ref[...], ((1,), (0,)))
    winds = [
        courant_limit * jnp.tanh(winds[t * z.block : (t + 1) * z.block]) for t in range(5)
    ]
    zonal, merid = winds[:2], winds[2:]

    sublane = lax.broadcasted_iota(jnp.int32, (z.block, z.lon), 0)
    low = sublane < z.levels
    level = sublane % z.levels

    def pair(a, b):
        return jnp.concatenate([a, b], axis=0)

    def swap(x):
        return pltpu.roll(x, z.levels, 0)

    def west(x):
        return pltpu.roll(x, 1, 1)

    def east(x):
        return pltpu.roll(x, z.lon - 1, 1)

    def around(south, centre, north):
        turn_s, turn_c, turn_n = swap(south), swap(centre), swap(north)
        inner = (jnp.where(low, turn_s, turn_c), centre, jnp.where(low, turn_c, turn_n))
        outer = (
            jnp.where(low, turn_c, turn_s),
            jnp.where(low, north, south),
            jnp.where(low, turn_n, turn_c),
        )
        return inner, outer

    def zonal_face(courant, flags):
        speed = 0.5 * (west(courant) + courant)
        magnitude = jnp.abs(speed)
        return 0.5 * speed, 0.5 * (magnitude - flags * (magnitude - speed * speed))

    def lat_faces(courants, first_row, second_row):
        faces = []
        for a, b, step in ((courants[0], courants[1], 0), (courants[1], courants[2], 1)):
            rows = [band * z.rows + row + step for row in (first_row, second_row)]
            is_open = [jnp.where((row > 0) & (row < lat_total), 0.5, 0.0) for row in rows]
            is_open = jnp.where(low, is_open[0], is_open[1])
            speed = 0.5 * (a + b)
            faces.append((speed * is_open, jnp.abs(speed) * is_open))
        return faces

    def horizontal(rows, zonal_face, lat_faces):
        south, centre, north = rows
        speed, diffuse = zonal_face
        western = west(centre)
        flux = speed * (western + centre) - diffuse * (centre - western)
        (speed_s, spread_s), (speed_n, spread_n) = lat_faces
        flux_s = speed_s * (south + centre) - spread_s * (centre - south)
        flux_n = speed_n * (centre + north) - spread_n * (north - centre)
        return -(east(flux) - flux) - (flux_n - flux_s)

    place = level_set * z.levels + level
    rise_low = jnp.where(place > 0, diffusivity, 0.0).astype(f32)
    rise_high = jnp.where(place + 1 < lev_total, diffusivity, 0.0).astype(f32)

    def vertical(x, below, above):
        down = jnp.where(level == 0, below, pltpu.roll(x, 1, 0))
        up = jnp.where(level == z.levels - 1, above, pltpu.roll(x, z.block - 1, 0))
        return rise_high * (up - x) - rise_low * (x - down)

    got = [by_parity("wave", first_ref[j], second_ref[j]) for j in range(z.rows + 1)]
    flags_inner = pair(own_ref[z.rows], own_ref[z.rows + 1])
    flags_outer = pair(got[z.rows][1], got[z.rows][0])
    centre = pair(own_ref[0], own_ref[1])
    inner, outer = around(pair(got[0][0], got[1][0]), centre, pair(got[0][1], got[1][1]))
    merid_inner, merid_outer = around(*merid)
    face_inner = zonal_face(zonal[0], flags_inner)
    face_outer = zonal_face(zonal[1], flags_outer)
    lat_inner = lat_faces(merid_inner, 0, 1)
    lat_outer = lat_faces(merid_outer, z.rows, -1)
    below, above = by_parity("lev", lev_first_ref[...], lev_second_ref[...])

    def halo_tile(rows, first, second):
        return jnp.where(low, rows[first : first + 1], rows[second : second + 1])

    s_inner = horizontal(inner, face_inner, lat_inner) + vertical(
        centre, halo_tile(below, 1, 2), halo_tile(above, 1, 2)
    )
    s_outer = horizontal(outer, face_outer, lat_outer) + vertical(
        outer[1], halo_tile(below, 3, 0), halo_tile(above, 3, 0)
    )
    turn_inner, turn_outer = swap(s_inner), swap(s_outer)
    rows = (
        jnp.where(low, turn_outer, turn_inner),
        s_inner,
        jnp.where(low, turn_inner, turn_outer),
    )
    change = s_inner + 0.5 * (
        horizontal(rows, face_inner, lat_inner) + vertical(s_inner, 0.0, 0.0)
    )
    tops, lows = [], []
    for x in (change, s_inner):
        top = x.astype(jnp.bfloat16).astype(f32)
        tops.append(top)
        lows.append(x - top)
    both = jnp.concatenate(tops + lows, axis=0).astype(jnp.bfloat16)
    projected = contract(both, table_ref[...], ((1,), (1,)))
    count = 2 * z.block
    scale = jnp.concatenate([scale_ref[:, :1]] * 2, axis=0)
    projected = (projected[:count] + projected[count:]) * scale
    top = projected.astype(jnp.bfloat16)
    both = jnp.concatenate([top, (projected - top.astype(f32)).astype(jnp.bfloat16)], axis=0)
    for b in range(z.bands):
        first = b * z.slot_pad
        block = jnp.concatenate(
            [both[:, p * height + first : p * height + first + z.slot_pad] for p in range(2)], axis=1
        )
        block = contract(block, spread_ref[...], ((1,), (0,)))
        block = block[:count] + block[count:]
        mine, edge = block[: z.block], block[z.block :]

        def by_row(x):
            return jnp.concatenate(
                [
                    jnp.sum(x[j * z.levels : (j + 1) * z.levels], axis=0, keepdims=True)
                    for j in range(z.rows)
                ],
                axis=0,
            )

        mine = by_row(mine * pick_ref[0])
        to_above, to_below = by_row(edge * pick_ref[1]), by_row(edge * pick_ref[2])
        for l in range(z.sets):
            reply = jnp.where(level_set == l, mine, 0.0)
            reply = jnp.where(level_set == l - 1, to_above, reply)
            reply_ref[b * z.sets + l] = jnp.where(level_set == l + 1, to_below, reply)


def analysis_kernel(z, arrived_ref, live_ref, out_ref, turned_ref):
    arrived = arrived_ref[:, 0]
    for l in range(1, z.sets):
        arrived = arrived + arrived_ref[:, l]
    arrived = arrived.reshape(z.lats, z.reply)
    top = arrived.astype(jnp.bfloat16).astype(jnp.float32)
    turned = jnp.concatenate([top, arrived - top], axis=0)
    width = turned_ref.shape[2]
    for c in range(turned_ref.shape[0]):
        turned_ref[c] = turned[c * width : (c + 1) * width].T
    height = 2 * z.levels
    for s in range(z.slots):
        left = [
            turned_ref[c, pl.ds(s, height, stride=z.slot_pad), :].astype(jnp.bfloat16)
            for c in range(turned_ref.shape[0])
        ]
        left = jnp.concatenate(left, axis=1)
        right = jnp.concatenate([live_ref[s], live_ref[s]], axis=0)
        out_ref[s] = contract(left, right, ((1,), (0,))).reshape(2, z.levels, z.degrees)


def in_hbm(array):
    return pltpu.with_memory_space_constraint(array, pltpu.HBM)


def nbytes(array, dtype=None):
    return array.size * jnp.dtype(dtype or array.dtype).itemsize


def swaps(axis):
    count = lax.axis_size(axis)
    pairs = [[(i, i + 1) for i in range(start, count - 1, 2)] for start in (0, 1)]
    return [p + [(b, a) for a, b in p] for p in pairs]


def on_device(spectra, legendre, derivative, tracer, limiter_flags, lat_weight, slot_wave):
    z = Sizes(spectra, legendre, tracer, lax.axis_size("wave"), lax.axis_size("lev"))
    f32, bf16 = jnp.float32, jnp.bfloat16
    fan = 4 * z.bands * z.sets * z.slot_pad * z.piece
    table_bytes = 4 * z.bands * z.slot_pad * z.lon
    any_spec = pl.BlockSpec(memory_space=pltpu.HBM)
    edge_shape = jax.ShapeDtypeStruct((z.rows + 1, z.levels, z.lon), f32)
    group_count = -(-z.slots * z.unit // lanes)
    fetched = (slot_wave, lat_weight, spectra, legendre, derivative, tracer, limiter_flags)
    pieces, live, scale, own, to_first, to_second = pl.pallas_call(
        functools.partial(legendre_kernel, z),
        name="legendre",
        in_specs=[any_spec] * len(fetched),
        out_specs=tuple(vmem(6)),
        out_shape=(
            jax.ShapeDtypeStruct((z.bands, z.slot_pad, z.piece), bf16),
            jax.ShapeDtypeStruct(legendre.shape, bf16),
            jax.ShapeDtypeStruct((z.block, lanes), f32),
            jax.ShapeDtypeStruct((2 * z.rows, z.levels, z.lon), f32),
            edge_shape,
            edge_shape,
        ),
        scratch_shapes=[pltpu.SMEM(x.shape, x.dtype) for x in fetched[:2]]
        + [pltpu.VMEM(x.shape, x.dtype) for x in fetched[2:]]
        + [
            pltpu.VMEM((z.slot_pad * z.lats, lanes), f32),
            pltpu.SemaphoreType.DMA((7, group_count)),
        ],
        compiler_params=params(
            2 * nbytes(spectra), 6 * nbytes(legendre), 8 * nbytes(tracer), fan
        ),
    )(*map(in_hbm, fetched))
    first_pairs, second_pairs = swaps("wave")
    wave_first = lax.ppermute(to_first, "wave", first_pairs)
    wave_second = lax.ppermute(to_second, "wave", second_pairs)
    arrived = lax.all_to_all(pieces, "wave", split_axis=0, concat_axis=0, tiled=True)
    padded_wave = jnp.pad(
        slot_wave.reshape(z.bands, z.slots), ((0, 0), (0, z.slot_pad - z.slots))
    ).reshape(-1, 1)
    table = pl.pallas_call(
        functools.partial(table_kernel, z),
        name="table",
        in_specs=vmem(1),
        out_specs=vmem(1)[0],
        out_shape=jax.ShapeDtypeStruct((2 * z.bands * z.slot_pad, z.lon), bf16),
        compiler_params=params(table_bytes),
    )(padded_wave)
    up_shape = jax.ShapeDtypeStruct((z.rows + 2, z.lon), f32)
    up, down = pl.pallas_call(
        functools.partial(edge_kernel, z),
        name="edges",
        in_specs=vmem(3),
        out_specs=tuple(vmem(2)),
        out_shape=(up_shape, up_shape),
        compiler_params=params(8 * nbytes(tracer)),
    )(own, wave_first, wave_second)
    first_pairs, second_pairs = swaps("lev")
    lev_first = lax.ppermute(up, "lev", first_pairs)
    lev_second = lax.ppermute(down, "lev", second_pairs)
    reply = pl.pallas_call(
        functools.partial(grid_kernel, z),
        name="grid",
        in_specs=vmem(11),
        out_specs=vmem(1)[0],
        out_shape=jax.ShapeDtypeStruct((z.bands * z.sets, z.rows, z.reply), f32),
        compiler_params=params(3 * table_bytes, 24 * nbytes(tracer), fan),
    )(
        arrived,
        unpack_constant(z),
        table,
        own,
        wave_first,
        wave_second,
        lev_first,
        lev_second,
        *reply_constants(z),
        scale,
    )
    returned = lax.all_to_all(reply, ("wave", "lev"), split_axis=0, concat_axis=0, tiled=True)
    width = math.gcd(2 * z.lats, lanes)
    return pl.pallas_call(
        functools.partial(analysis_kernel, z),
        name="analysis",
        in_specs=vmem(2),
        out_specs=vmem(1)[0],
        out_shape=jax.ShapeDtypeStruct((z.slots, 2, z.levels, z.degrees), f32),
        scratch_shapes=[pltpu.VMEM((2 * z.lats // width, z.reply, width), f32)],
        compiler_params=params(nbytes(spectra, f32), nbytes(legendre)),
    )(returned.reshape(z.bands, z.sets, z.rows, z.reply), live)


def solution(mesh):
    return jax.shard_map(
        on_device,
        mesh=mesh,
        in_specs=(
            P("wave", None, "lev", None),
            P("wave", None, None),
            P("wave", None, None),
            P("lev", "wave", None),
            P("lev", "wave", None),
            P("wave"),
            P(),
        ),
        out_specs=P("wave", None, "lev", None),
        check_vma=False,
    )
```

```python
import functools
import math

import jax
import jax.numpy as jnp
import numpy as np
from jax import lax
from jax.experimental import pallas as pl
from jax.experimental.pallas import tpu as pltpu
from jax.sharding import PartitionSpec as P

diffusivity = 0.15
courant_limit = 0.45
halo = 2
lanes = 128
packed_rows = 16
store_slots = 4


def round_up(value, step):
    return -(-value // step) * step


def contract(left, right, dims):
    return lax.dot_general(left, right, (dims, ((), ())), preferred_element_type=jnp.float32)


def vmem(count):
    return [pl.BlockSpec(memory_space=pltpu.VMEM)] * count


def params(*byte_counts):
    return pltpu.CompilerParams(vmem_limit_bytes=min(60 * 2**20, 6 * 2**20 + sum(byte_counts)))


class Sizes:
    def __init__(self, spectra, legendre, tracer, bands, sets):
        self.slots, _, self.levels, self.degrees = spectra.shape
        self.lats = legendre.shape[1]
        self.rows, self.lon = tracer.shape[1:]
        self.bands, self.sets = bands, sets
        self.order = [(bands // 2 + 1 - b) % bands for b in range(bands)]
        self.slot_pad = round_up(self.slots, packed_rows)
        self.window = self.rows + 2 * halo
        self.deep = self.levels + 2 * halo
        self.unit = 4 * self.levels
        self.piece = round_up(self.window * self.unit, lanes)
        self.stack = round_up(self.window * self.deep, 8)
        self.reply = round_up(2 * self.levels * self.slot_pad, lanes)
        assert self.rows == halo and self.deep == 8 and self.lon % lanes == 0
        assert lanes % self.unit == 0 and self.lats % 8 == 0


def piece_lanes(z):
    at = np.arange(z.piece)
    row, channel, level = at // z.unit, at // z.levels % 4, at % z.levels
    return channel % 2, channel // 2, row, level, row < z.window


def unpack_constant(z):
    part, wind, row, level, valid = piece_lanes(z)
    height = round_up(2 * z.stack, lanes)
    target = np.arange(2 * height)
    t_part, rest = target // height, target % height
    t_wind, rest = rest // z.stack, rest % z.stack
    t_row, t_deep = rest // z.deep, rest % z.deep
    t_valid = (t_wind < 2) & (t_row < z.window)
    same = (t_part[:, None] == part) & (t_wind[:, None] == wind) & (t_row[:, None] == row)
    same = same & valid & t_valid[:, None]
    own = same & (t_deep[:, None] == level + halo)
    below = same & (t_deep[:, None] == halo - 1) & (level == z.levels - 1)
    above = same & (t_deep[:, None] == halo + z.levels) & (level == 0)
    return jnp.asarray(np.concatenate([own, below, above], axis=1), jnp.bfloat16)


def reply_constants(z):
    at = np.arange(z.reply)
    part, rest = at // (z.levels * z.slot_pad), at % (z.levels * z.slot_pad)
    level, slot = rest // z.slot_pad, rest % z.slot_pad
    source = np.arange(2 * z.slot_pad)
    spread = (source[:, None] // z.slot_pad == part) & (source[:, None] % z.slot_pad == slot)
    pick = np.arange(z.deep)[:, None] == level + halo
    return jnp.asarray(spread, jnp.bfloat16), pick.astype(np.float32)


def legendre_kernel(
    z,
    wave_hbm,
    weight_hbm,
    spectra_hbm,
    legendre_hbm,
    derivative_hbm,
    tracer_hbm,
    flags_hbm,
    pieces_ref,
    live_ref,
    scale_ref,
    own_ref,
    first_ref,
    second_ref,
    wave_ref,
    weight_ref,
    spectra_ref,
    legendre_ref,
    derivative_ref,
    tracer_ref,
    flags_ref,
    by_slot_ref,
    sems,
):
    group_slots = lanes // z.unit
    groups = [
        (first, min(first + group_slots, z.slots)) for first in range(0, z.slots, group_slots)
    ]
    whole = [
        pltpu.make_async_copy(hbm, ref, sems.at[a, 0])
        for a, (hbm, ref) in enumerate(
            (
                (wave_hbm, wave_ref),
                (weight_hbm, weight_ref),
                (tracer_hbm, tracer_ref),
                (flags_hbm, flags_ref),
            )
        )
    ]
    fetches = []
    for g, (first, last) in enumerate(groups):
        part = pl.ds(first, last - first)
        fetches.append(
            [
                pltpu.make_async_copy(hbm.at[part], ref.at[part], sems.at[4 + a, g])
                for a, (hbm, ref) in enumerate(
                    (
                        (legendre_hbm, legendre_ref),
                        (derivative_hbm, derivative_ref),
                        (spectra_hbm, spectra_ref),
                    )
                )
            ]
        )
    for copies in [whole[:2], *fetches, whole[2:]]:
        for copy in copies:
            copy.start()
    base = lax.axis_index("wave") * z.slots
    by_slot_ref[...] = jnp.zeros_like(by_slot_ref)
    whole[0].wait()
    whole[1].wait()
    for j in range(z.rows):
        scale = weight_ref[j] * (1.0 / math.sqrt(z.lon))
        scale_ref[j * z.deep : (j + 1) * z.deep] = jnp.full((z.deep, lanes), scale, jnp.float32)
    degree = lax.broadcasted_iota(jnp.int32, (z.lats, z.degrees), 1)
    lane = lax.broadcasted_iota(jnp.int32, (z.lats, lanes), 1)
    lane_slot, channel = lane // z.unit, lane // z.levels % 4
    sign_sum = jnp.where(channel % 2 == 0, -1.0, 1.0)
    sign_slope = jnp.where(channel < 2, -1.0, 1.0)
    for (first, last), copies in zip(groups, fetches):
        waves = [wave_ref[base + s] for s in range(first, last)]
        for copy in copies:
            copy.wait()
        sums, slopes = [], []
        for s, wave in zip(range(first, last), waves):
            live = jnp.where(degree >= wave, 1.0, 0.0).astype(jnp.bfloat16)
            masked = legendre_ref[s] * live
            live_ref[s] = masked
            sums.append(masked)
            slopes.append(derivative_ref[s] * live)
        right = [spectra_ref[s].reshape(z.unit, z.degrees) for s in range(first, last)]
        right += [jnp.zeros_like(right[0])] * (group_slots - len(right))
        right = jnp.concatenate(right, axis=0)
        sums = contract(jnp.concatenate(sums, axis=0), right, ((1,), (1,)))
        slopes = contract(jnp.concatenate(slopes, axis=0), right, ((1,), (1,)))
        sum_of = jnp.zeros((z.lats, lanes), jnp.float32)
        slope_of = sum_of
        factor = sum_of
        doubled = sum_of
        for at, wave in enumerate(waves):
            mine = lane_slot == at
            block = slice(at * z.lats, (at + 1) * z.lats)
            sum_of = jnp.where(mine, sums[block], sum_of)
            slope_of = jnp.where(mine, slopes[block], slope_of)
            factor = jnp.where(mine, wave.astype(jnp.float32) / z.degrees, factor)
            doubled = jnp.where(mine, jnp.where(wave == 0, 1.0, 2.0), doubled)
        turned = sum_of
        for c in range(4):
            moved = pltpu.roll(sum_of, (2 * c - 3) * z.levels % lanes, 1)
            turned = jnp.where(channel == c, moved, turned)
        winds = (factor * sign_sum * turned + sign_slope * slope_of) * doubled
        for at, s in enumerate(range(first, last)):
            moved = winds if at == 0 else pltpu.roll(winds, lanes - at * z.unit, 1)
            by_slot_ref[s * z.lats : (s + 1) * z.lats] = moved
    tiles = round_up((z.lats + 2 * halo) * z.unit, lanes) // lanes + z.piece // lanes
    rows = [jnp.zeros((z.slot_pad, lanes), jnp.float32) for _ in range(tiles)]
    slot_lane = lax.broadcasted_iota(jnp.int32, (z.slot_pad, lanes), 1) // z.unit
    for lat in range(z.lats):
        tile, at = divmod((lat + halo) * z.unit, lanes)
        block = by_slot_ref[pl.ds(lat, z.slot_pad, stride=z.lats), :]
        block = block if at == 0 else pltpu.roll(block, at, 1)
        rows[tile] = jnp.where(slot_lane == at // z.unit, block, rows[tile])
    rows = jnp.concatenate(rows, axis=1)
    for b in range(z.bands):
        at = b * z.rows * z.unit
        piece = rows[:, at : at + z.piece].astype(jnp.bfloat16)
        for l in range(z.sets):
            pieces_ref[b * z.sets + l] = piece

    even = lax.axis_index("wave") % 2 == 0
    whole[2].wait()
    for j in range(z.rows):
        row = tracer_ref[:, j, :]
        own_ref[j] = row
        first_ref[j] = row
        second_ref[j] = row
    whole[3].wait()
    switched = [flags_ref[:, j, :].astype(jnp.float32) for j in range(z.rows)]
    for j in range(z.rows):
        own_ref[z.rows + j] = switched[j]
    first_ref[z.rows] = jnp.where(even, switched[-1], switched[0])
    second_ref[z.rows] = jnp.where(even, switched[0], switched[-1])


def table_kernel(z, wave_ref, table_ref):
    wave = wave_ref[...].astype(jnp.float32)
    height = wave.shape[0]
    chunks = z.lon // lanes
    at = lax.broadcasted_iota(jnp.int32, (height, lanes), 1).astype(jnp.float32)

    def parts(phase):
        phase = phase - jnp.floor(phase * (1.0 / z.lon) + 0.5) * z.lon
        angle = phase * (2.0 * math.pi / z.lon)
        return jnp.cos(angle), jnp.sin(angle)

    fine_cos, fine_sin = parts(wave * at)
    coarse = [parts(wave * ((at + b) * lanes)) for b in range(0, chunks, lanes)]
    for a in range(chunks):
        cos_a = coarse[a // lanes][0][:, a % lanes : a % lanes + 1]
        sin_a = coarse[a // lanes][1][:, a % lanes : a % lanes + 1]
        columns = slice(a * lanes, (a + 1) * lanes)
        table_ref[:height, columns] = (cos_a * fine_cos - sin_a * fine_sin).astype(jnp.bfloat16)
        table_ref[height:, columns] = (-(sin_a * fine_cos + cos_a * fine_sin)).astype(jnp.bfloat16)


def by_parity(axis, first, second):
    even = lax.axis_index(axis) % 2 == 0
    return jnp.where(even, second, first), jnp.where(even, first, second)


def edge_kernel(z, own_ref, first_ref, second_ref, up_ref, down_ref):
    south, _ = by_parity("wave", first_ref[z.rows - 1], second_ref[z.rows - 1])
    _, north = by_parity("wave", first_ref[0], second_ref[0])
    even = lax.axis_index("lev") % 2 == 0
    rows = [south] + [own_ref[j] for j in range(z.rows)] + [north]
    plan = [(row, z.levels - 1, 0) for row in rows]
    plan += [(row, z.levels - 2, 1) for row in rows[1:-1]]
    plan += [(own_ref[z.rows + j], z.levels - 1, 0) for j in range(z.rows)]
    for at, (row, top, bottom) in enumerate(plan):
        top, bottom = row[top : top + 1], row[bottom : bottom + 1]
        up_ref[at : at + 1] = jnp.where(even, top, bottom)
        down_ref[at : at + 1] = jnp.where(even, bottom, top)


def grid_kernel(
    z,
    arrived_ref,
    unpack_ref,
    table_ref,
    own_ref,
    first_ref,
    second_ref,
    lev_first_ref,
    lev_second_ref,
    spread_ref,
    pick_ref,
    scale_ref,
    reply_ref,
    q_ref,
    f_ref,
):
    band, level_set = lax.axis_index("wave"), lax.axis_index("lev")
    lat_total = z.bands * z.rows
    lev_total = z.sets * z.levels
    own = slice(halo, halo + z.levels)
    q_ref[...] = jnp.zeros_like(q_ref)
    f_ref[...] = jnp.zeros_like(f_ref)
    for j in range(halo):
        south, north = by_parity("wave", first_ref[j], second_ref[j])
        q_ref[j, own] = south
        q_ref[halo + z.rows + j, own] = north
    south, north = by_parity("wave", first_ref[z.rows], second_ref[z.rows])
    f_ref[0, own] = south
    f_ref[z.rows + 1, own] = north
    for j in range(z.rows):
        q_ref[halo + j, own] = own_ref[j]
        f_ref[1 + j, own] = own_ref[z.rows + j]
    below, above = by_parity("lev", lev_first_ref[...], lev_second_ref[...])
    for got, near, far in ((below, halo - 1, 0), (above, halo + z.levels, z.deep - 1)):
        for j in range(z.rows + 2):
            q_ref[halo - 1 + j, near : near + 1] = got[j : j + 1]
        for j in range(z.rows):
            at = z.rows + 2 + j
            q_ref[halo + j, far : far + 1] = got[at : at + 1]
            at = 2 * z.rows + 2 + j
            f_ref[1 + j, near : near + 1] = got[at : at + 1]

    height = z.bands * z.slot_pad

    def from_set(index):
        return arrived_ref[:, index].reshape(height, z.piece)

    blocks = jnp.concatenate(
        [
            from_set(level_set),
            from_set(jnp.maximum(level_set - 1, 0)),
            from_set(jnp.minimum(level_set + 1, z.sets - 1)),
        ],
        axis=1,
    )
    turned = contract(unpack_ref[...], blocks, ((1,), (1,))).astype(jnp.bfloat16)
    span = turned.shape[0] // 2
    turned = jnp.concatenate([turned[:span], turned[span:]], axis=1)
    winds = contract(turned, table_ref[...], ((1,), (0,)))

    def wind(which, j):
        first = which * z.stack + j * z.deep
        return courant_limit * jnp.tanh(winds[first : first + z.deep])

    zonal = [wind(0, j) for j in range(1, z.rows + 3)]
    merid = [wind(1, j) for j in range(z.window)]

    def west(x):
        return pltpu.roll(x, 1, 1)

    def east(x):
        return pltpu.roll(x, z.lon - 1, 1)

    face = []
    for j in range(z.rows + 2):
        speed = 0.5 * (west(zonal[j]) + zonal[j])
        magnitude = jnp.abs(speed)
        diffuse = 0.5 * (magnitude - f_ref[j] * (magnitude - speed * speed))
        face.append((speed, diffuse))
    lat_face = []
    for j in range(1, z.window):
        index = band * z.rows - halo + j
        is_open = jnp.where((index > 0) & (index < lat_total), 0.5, 0.0).astype(jnp.float32)
        speed = 0.5 * (merid[j - 1] + merid[j])
        lat_face.append((speed * is_open, jnp.abs(speed) * is_open))
    deep = lax.broadcasted_iota(jnp.int32, (z.deep, z.lon), 0) + (level_set * z.levels - halo)
    rise = jnp.where((deep > 0) & (deep < lev_total), diffusivity, 0.0).astype(jnp.float32)

    def tendency(q, first):
        north_flux = []
        for j in range(len(q) - 1):
            mean, spread = lat_face[first - 1 + j]
            north_flux.append(mean * (q[j] + q[j + 1]) - spread * (q[j + 1] - q[j]))
        result = []
        for j in range(1, len(q) - 1):
            speed, diffuse = face[first - 2 + j]
            centre = q[j]
            western = west(centre)
            flux = speed * 0.5 * (western + centre) - diffuse * (centre - western)
            lift = rise * (centre - pltpu.roll(centre, 1, 0))
            result.append(
                -(east(flux) - flux)
                - (north_flux[j] - north_flux[j - 1])
                + (pltpu.roll(lift, z.deep - 1, 0) - lift)
            )
        return result

    tracer = [q_ref[j] for j in range(z.window)]
    first_tendency = tendency(tracer, 1)
    section_one = [q + t for q, t in zip(tracer[1:-1], first_tendency)]
    section_two = tendency(section_one, 2)
    tops, lows = [], []
    for j in range(z.rows):
        q = tracer[halo + j]
        change = 0.5 * q + 0.5 * (section_one[1 + j] + section_two[j]) - q
        top = change.astype(jnp.bfloat16)
        tops.append(top.astype(jnp.float32))
        lows.append(change - tops[-1])
    both = jnp.concatenate(tops + lows, axis=0).astype(jnp.bfloat16)
    projected = contract(both, table_ref[...], ((1,), (1,)))
    count = z.rows * z.deep
    projected = projected[:count] + projected[count:]
    scaled = projected * scale_ref[:, :1]
    top = scaled.astype(jnp.bfloat16)
    low = (scaled - top.astype(jnp.float32)).astype(jnp.bfloat16)
    both = jnp.concatenate([top, low], axis=0)

    def of_band(b):
        first = b * z.slot_pad
        halves = [both[:, p * height + first : p * height + first + z.slot_pad] for p in range(2)]
        return jnp.concatenate(halves, axis=1)

    spread = jnp.concatenate([of_band(b) for b in range(z.bands)], axis=0)
    spread = contract(spread, spread_ref[...], ((1,), (0,)))
    for b in range(z.bands):
        block = spread[2 * b * count : 2 * (b + 1) * count]
        block = block[:count] + block[count:]
        for j in range(z.rows):
            mine = block[j * z.deep : (j + 1) * z.deep] * pick_ref[...]
            reply_ref[z.order.index(b), j : j + 1] = jnp.sum(mine, axis=0, keepdims=True)


def analysis_kernel(z, arrived_ref, live_ref, out_hbm, turned_ref, out_ref, sems):
    arrived = [arrived_ref[z.order.index(b)] for b in range(z.bands)]
    arrived = jnp.concatenate(arrived, axis=0)
    top = arrived.astype(jnp.bfloat16).astype(jnp.float32)
    turned = jnp.concatenate([top, arrived - top], axis=0)
    width = turned_ref.shape[2]
    for c in range(turned_ref.shape[0]):
        turned_ref[c] = turned[c * width : (c + 1) * width].T
    height = 2 * z.levels
    stores = []
    for s in range(z.slots):
        left = [
            turned_ref[c, pl.ds(s, height, stride=z.slot_pad), :].astype(jnp.bfloat16)
            for c in range(turned_ref.shape[0])
        ]
        left = jnp.concatenate(left, axis=1)
        right = jnp.concatenate([live_ref[s], live_ref[s]], axis=0)
        out_ref[s] = contract(left, right, ((1,), (0,))).reshape(2, z.levels, z.degrees)
        if s % store_slots == store_slots - 1 or s == z.slots - 1:
            first = s // store_slots * store_slots
            part = pl.ds(first, s + 1 - first)
            stores.append(
                pltpu.make_async_copy(out_ref.at[part], out_hbm.at[part], sems.at[len(stores)])
            )
            stores[-1].start()
    for store in stores:
        store.wait()


def in_hbm(array):
    return pltpu.with_memory_space_constraint(array, pltpu.HBM)


def nbytes(array, dtype=None):
    return array.size * jnp.dtype(dtype or array.dtype).itemsize


def swaps(axis):
    count = lax.axis_size(axis)
    pairs = [[(i, i + 1) for i in range(start, count - 1, 2)] for start in (0, 1)]
    return [p + [(b, a) for a, b in p] for p in pairs]


def on_device(spectra, legendre, derivative, tracer, limiter_flags, lat_weight, slot_wave):
    z = Sizes(spectra, legendre, tracer, lax.axis_size("wave"), lax.axis_size("lev"))
    f32, bf16 = jnp.float32, jnp.bfloat16
    fan = 4 * z.bands * z.sets * z.slot_pad * z.piece
    table_bytes = 4 * z.bands * z.slot_pad * z.lon
    any_spec = pl.BlockSpec(memory_space=pltpu.HBM)
    edge_shape = jax.ShapeDtypeStruct((z.rows + 1, z.levels, z.lon), f32)
    group_count = -(-z.slots * z.unit // lanes)
    fetched = (slot_wave, lat_weight, spectra, legendre, derivative, tracer, limiter_flags)
    pieces, live, scale, own, to_first, to_second = pl.pallas_call(
        functools.partial(legendre_kernel, z),
        name="legendre",
        in_specs=[any_spec] * len(fetched),
        out_specs=tuple(vmem(6)),
        out_shape=(
            jax.ShapeDtypeStruct((z.bands * z.sets, z.slot_pad, z.piece), bf16),
            jax.ShapeDtypeStruct(legendre.shape, bf16),
            jax.ShapeDtypeStruct((z.rows * z.deep, lanes), f32),
            jax.ShapeDtypeStruct((2 * z.rows, z.levels, z.lon), f32),
            edge_shape,
            edge_shape,
        ),
        scratch_shapes=[pltpu.SMEM(x.shape, x.dtype) for x in fetched[:2]]
        + [pltpu.VMEM(x.shape, x.dtype) for x in fetched[2:]]
        + [
            pltpu.VMEM((z.slot_pad * z.lats, lanes), f32),
            pltpu.SemaphoreType.DMA((7, group_count)),
        ],
        compiler_params=params(
            2 * nbytes(spectra), 6 * nbytes(legendre), 8 * nbytes(tracer), fan
        ),
    )(*map(in_hbm, fetched))
    first_pairs, second_pairs = swaps("wave")
    wave_first = lax.ppermute(to_first, "wave", first_pairs)
    wave_second = lax.ppermute(to_second, "wave", second_pairs)
    arrived = lax.all_to_all(pieces, ("wave", "lev"), split_axis=0, concat_axis=0, tiled=True)
    padded_wave = jnp.pad(
        slot_wave.reshape(z.bands, z.slots), ((0, 0), (0, z.slot_pad - z.slots))
    ).reshape(-1, 1)
    table = pl.pallas_call(
        functools.partial(table_kernel, z),
        name="table",
        in_specs=vmem(1),
        out_specs=vmem(1)[0],
        out_shape=jax.ShapeDtypeStruct((2 * z.bands * z.slot_pad, z.lon), bf16),
        compiler_params=params(table_bytes),
    )(padded_wave)
    up_shape = jax.ShapeDtypeStruct((3 * z.rows + 2, z.lon), f32)
    up, down = pl.pallas_call(
        functools.partial(edge_kernel, z),
        name="edges",
        in_specs=vmem(3),
        out_specs=tuple(vmem(2)),
        out_shape=(up_shape, up_shape),
        compiler_params=params(8 * nbytes(tracer)),
    )(own, wave_first, wave_second)
    first_pairs, second_pairs = swaps("lev")
    lev_first = lax.ppermute(up, "lev", first_pairs)
    lev_second = lax.ppermute(down, "lev", second_pairs)
    reply = pl.pallas_call(
        functools.partial(grid_kernel, z),
        name="grid",
        in_specs=vmem(11),
        out_specs=vmem(1)[0],
        out_shape=jax.ShapeDtypeStruct((z.bands, z.rows, z.reply), f32),
        scratch_shapes=[
            pltpu.VMEM((z.window, z.deep, z.lon), f32),
            pltpu.VMEM((z.rows + 2, z.deep, z.lon), f32),
        ],
        compiler_params=params(3 * table_bytes, 24 * nbytes(tracer), fan),
    )(
        arrived.reshape(z.bands, z.sets, z.slot_pad, z.piece),
        unpack_constant(z),
        table,
        own,
        wave_first,
        wave_second,
        lev_first,
        lev_second,
        *reply_constants(z),
        scale,
    )
    returned = lax.all_to_all(
        reply, "wave", split_axis=0, concat_axis=0, axis_index_groups=[z.order], tiled=True
    )
    width = math.gcd(2 * z.lats, lanes)
    return pl.pallas_call(
        functools.partial(analysis_kernel, z),
        name="analysis",
        in_specs=vmem(2),
        out_specs=any_spec,
        out_shape=jax.ShapeDtypeStruct((z.slots, 2, z.levels, z.degrees), f32),
        scratch_shapes=[
            pltpu.VMEM((2 * z.lats // width, z.reply, width), f32),
            pltpu.VMEM((z.slots, 2, z.levels, z.degrees), f32),
            pltpu.SemaphoreType.DMA((-(-z.slots // store_slots),)),
        ],
        compiler_params=params(nbytes(spectra, f32), nbytes(legendre)),
    )(returned, live)


def solution(mesh):
    return jax.shard_map(
        on_device,
        mesh=mesh,
        in_specs=(
            P("wave", None, "lev", None),
            P("wave", None, None),
            P("wave", None, None),
            P("lev", "wave", None),
            P("lev", "wave", None),
            P("wave"),
            P(),
        ),
        out_specs=P("wave", None, "lev", None),
        check_vma=False,
    )
```

```python
import functools
import math

import jax
import jax.numpy as jnp
import numpy as np
from jax import lax
from jax.experimental import pallas as pl
from jax.experimental.pallas import tpu as pltpu
from jax.sharding import PartitionSpec as P

diffusivity = 0.15
courant_limit = 0.45
halo = 2
lanes = 128
packed_rows = 16
store_slots = 4


def round_up(value, step):
    return -(-value // step) * step


def contract(left, right, dims):
    return lax.dot_general(left, right, (dims, ((), ())), preferred_element_type=jnp.float32)


def vmem(count):
    return [pl.BlockSpec(memory_space=pltpu.VMEM)] * count


def params(*byte_counts):
    return pltpu.CompilerParams(vmem_limit_bytes=min(60 * 2**20, 6 * 2**20 + sum(byte_counts)))


class Sizes:
    def __init__(self, spectra, legendre, tracer, bands, sets):
        self.slots, _, self.levels, self.degrees = spectra.shape
        self.lats = legendre.shape[1]
        self.rows, self.lon = tracer.shape[1:]
        self.bands, self.sets = bands, sets
        self.order = [(bands // 2 + 1 - b) % bands for b in range(bands)]
        self.slot_pad = round_up(self.slots, packed_rows)
        self.window = self.rows + 2 * halo
        self.deep = self.levels + 2 * halo
        self.unit = 4 * self.levels
        self.piece = round_up(self.window * self.unit, lanes)
        self.stack = round_up(self.window * self.deep, 8)
        self.reply = round_up(2 * self.levels * self.slot_pad, lanes)
        assert self.rows == halo and self.deep == 8 and self.lon % lanes == 0
        assert lanes % self.unit == 0 and self.lats % 8 == 0


def piece_lanes(z):
    at = np.arange(z.piece)
    row, channel, level = at // z.unit, at // z.levels % 4, at % z.levels
    return channel % 2, channel // 2, row, level, row < z.window


def unpack_constant(z):
    part, wind, row, level, valid = piece_lanes(z)
    height = round_up(2 * z.stack, lanes)
    target = np.arange(2 * height)
    t_part, rest = target // height, target % height
    t_wind, rest = rest // z.stack, rest % z.stack
    t_row, t_deep = rest // z.deep, rest % z.deep
    t_valid = (t_wind < 2) & (t_row < z.window)
    same = (t_part[:, None] == part) & (t_wind[:, None] == wind) & (t_row[:, None] == row)
    same = same & valid & t_valid[:, None]
    own = same & (t_deep[:, None] == level + halo)
    below = same & (t_deep[:, None] == halo - 1) & (level == z.levels - 1)
    above = same & (t_deep[:, None] == halo + z.levels) & (level == 0)
    return jnp.asarray(np.concatenate([own, below, above], axis=1), jnp.bfloat16)


def reply_constants(z):
    at = np.arange(z.reply)
    part, rest = at // (z.levels * z.slot_pad), at % (z.levels * z.slot_pad)
    level, slot = rest // z.slot_pad, rest % z.slot_pad
    source = np.arange(2 * z.slot_pad)
    spread = (source[:, None] // z.slot_pad == part) & (source[:, None] % z.slot_pad == slot)
    pick = np.arange(z.deep)[:, None] == level + halo
    return jnp.asarray(spread, jnp.bfloat16), pick.astype(np.float32)


def legendre_kernel(
    z,
    wave_hbm,
    weight_hbm,
    spectra_hbm,
    legendre_hbm,
    derivative_hbm,
    tracer_hbm,
    flags_hbm,
    pieces_ref,
    live_ref,
    scale_ref,
    own_ref,
    first_ref,
    second_ref,
    wave_ref,
    weight_ref,
    spectra_ref,
    legendre_ref,
    derivative_ref,
    tracer_ref,
    flags_ref,
    by_slot_ref,
    sems,
):
    group_slots = lanes // z.unit
    groups = [
        (first, min(first + group_slots, z.slots)) for first in range(0, z.slots, group_slots)
    ]
    whole = [
        pltpu.make_async_copy(hbm, ref, sems.at[a, 0])
        for a, (hbm, ref) in enumerate(
            (
                (wave_hbm, wave_ref),
                (weight_hbm, weight_ref),
                (tracer_hbm, tracer_ref),
                (flags_hbm, flags_ref),
            )
        )
    ]
    fetches = [
        [
            pltpu.make_async_copy(hbm, ref, sems.at[4 + a, 0])
            for a, (hbm, ref) in enumerate(
                (
                    (spectra_hbm, spectra_ref),
                    (legendre_hbm, legendre_ref),
                    (derivative_hbm, derivative_ref),
                )
            )
        ]
    ] + [[] for _ in groups[1:]]
    for copies in [*fetches, whole]:
        for copy in copies:
            copy.start()
    base = lax.axis_index("wave") * z.slots
    by_slot_ref[...] = jnp.zeros_like(by_slot_ref)
    whole[0].wait()
    whole[1].wait()
    for j in range(z.rows):
        scale = weight_ref[j] * (1.0 / math.sqrt(z.lon))
        scale_ref[j * z.deep : (j + 1) * z.deep] = jnp.full((z.deep, lanes), scale, jnp.float32)
    degree = lax.broadcasted_iota(jnp.int32, (z.lats, z.degrees), 1)
    lane = lax.broadcasted_iota(jnp.int32, (z.lats, lanes), 1)
    lane_slot, channel = lane // z.unit, lane // z.levels % 4
    sign_sum = jnp.where(channel % 2 == 0, -1.0, 1.0)
    sign_slope = jnp.where(channel < 2, -1.0, 1.0)
    for (first, last), copies in zip(groups, fetches):
        waves = [wave_ref[base + s] for s in range(first, last)]
        for copy in copies:
            copy.wait()
        sums, slopes = [], []
        for s, wave in zip(range(first, last), waves):
            live = jnp.where(degree >= wave, 1.0, 0.0).astype(jnp.bfloat16)
            masked = legendre_ref[s] * live
            live_ref[s] = masked
            sums.append(masked)
            slopes.append(derivative_ref[s] * live)
        right = [spectra_ref[s].reshape(z.unit, z.degrees) for s in range(first, last)]
        right += [jnp.zeros_like(right[0])] * (group_slots - len(right))
        right = jnp.concatenate(right, axis=0)
        sums = contract(jnp.concatenate(sums, axis=0), right, ((1,), (1,)))
        slopes = contract(jnp.concatenate(slopes, axis=0), right, ((1,), (1,)))
        sum_of = jnp.zeros((z.lats, lanes), jnp.float32)
        slope_of = sum_of
        factor = sum_of
        doubled = sum_of
        for at, wave in enumerate(waves):
            mine = lane_slot == at
            block = slice(at * z.lats, (at + 1) * z.lats)
            sum_of = jnp.where(mine, sums[block], sum_of)
            slope_of = jnp.where(mine, slopes[block], slope_of)
            factor = jnp.where(mine, wave.astype(jnp.float32) / z.degrees, factor)
            doubled = jnp.where(mine, jnp.where(wave == 0, 1.0, 2.0), doubled)
        turned = sum_of
        for c in range(4):
            moved = pltpu.roll(sum_of, (2 * c - 3) * z.levels % lanes, 1)
            turned = jnp.where(channel == c, moved, turned)
        winds = (factor * sign_sum * turned + sign_slope * slope_of) * doubled
        for at, s in enumerate(range(first, last)):
            moved = winds if at == 0 else pltpu.roll(winds, lanes - at * z.unit, 1)
            by_slot_ref[s * z.lats : (s + 1) * z.lats] = moved
    tiles = round_up((z.lats + 2 * halo) * z.unit, lanes) // lanes + z.piece // lanes
    rows = [jnp.zeros((z.slot_pad, lanes), jnp.float32) for _ in range(tiles)]
    slot_lane = lax.broadcasted_iota(jnp.int32, (z.slot_pad, lanes), 1) // z.unit
    for lat in range(z.lats):
        tile, at = divmod((lat + halo) * z.unit, lanes)
        block = by_slot_ref[pl.ds(lat, z.slot_pad, stride=z.lats), :]
        block = block if at == 0 else pltpu.roll(block, at, 1)
        rows[tile] = jnp.where(slot_lane == at // z.unit, block, rows[tile])
    rows = jnp.concatenate(rows, axis=1)
    for b in range(z.bands):
        at = b * z.rows * z.unit
        piece = rows[:, at : at + z.piece].astype(jnp.bfloat16)
        for l in range(z.sets):
            pieces_ref[z.bands * z.sets - 1 - (b * z.sets + l)] = piece

    even = lax.axis_index("wave") % 2 == 0
    whole[2].wait()
    for j in range(z.rows):
        row = tracer_ref[:, j, :]
        own_ref[j] = row
        first_ref[j] = row
        second_ref[j] = row
    whole[3].wait()
    switched = [flags_ref[:, j, :].astype(jnp.float32) for j in range(z.rows)]
    for j in range(z.rows):
        own_ref[z.rows + j] = switched[j]
    first_ref[z.rows] = jnp.where(even, switched[-1], switched[0])
    second_ref[z.rows] = jnp.where(even, switched[0], switched[-1])


def table_kernel(z, wave_ref, table_ref):
    wave = wave_ref[...].astype(jnp.float32)
    height = wave.shape[0]
    chunks = z.lon // lanes
    at = lax.broadcasted_iota(jnp.int32, (height, lanes), 1).astype(jnp.float32)

    def parts(phase):
        phase = phase - jnp.floor(phase * (1.0 / z.lon) + 0.5) * z.lon
        angle = phase * (2.0 * math.pi / z.lon)
        return jnp.cos(angle), jnp.sin(angle)

    fine_cos, fine_sin = parts(wave * at)
    coarse = [parts(wave * ((at + b) * lanes)) for b in range(0, chunks, lanes)]
    for a in range(chunks):
        cos_a = coarse[a // lanes][0][:, a % lanes : a % lanes + 1]
        sin_a = coarse[a // lanes][1][:, a % lanes : a % lanes + 1]
        columns = slice(a * lanes, (a + 1) * lanes)
        table_ref[:height, columns] = (cos_a * fine_cos - sin_a * fine_sin).astype(jnp.bfloat16)
        table_ref[height:, columns] = (-(sin_a * fine_cos + cos_a * fine_sin)).astype(jnp.bfloat16)


def by_parity(axis, first, second):
    even = lax.axis_index(axis) % 2 == 0
    return jnp.where(even, second, first), jnp.where(even, first, second)


def edge_kernel(z, own_ref, first_ref, second_ref, up_ref, down_ref):
    south, _ = by_parity("wave", first_ref[z.rows - 1], second_ref[z.rows - 1])
    _, north = by_parity("wave", first_ref[0], second_ref[0])
    even = lax.axis_index("lev") % 2 == 0
    rows = [south] + [own_ref[j] for j in range(z.rows)] + [north]
    plan = [(row, z.levels - 1, 0) for row in rows]
    plan += [(row, z.levels - 2, 1) for row in rows[1:-1]]
    plan += [(own_ref[z.rows + j], z.levels - 1, 0) for j in range(z.rows)]
    for at, (row, top, bottom) in enumerate(plan):
        top, bottom = row[top : top + 1], row[bottom : bottom + 1]
        up_ref[at : at + 1] = jnp.where(even, top, bottom)
        down_ref[at : at + 1] = jnp.where(even, bottom, top)


def grid_kernel(
    z,
    arrived_ref,
    unpack_ref,
    table_ref,
    own_ref,
    first_ref,
    second_ref,
    lev_first_ref,
    lev_second_ref,
    spread_ref,
    pick_ref,
    scale_ref,
    reply_ref,
    q_ref,
    f_ref,
):
    band, level_set = lax.axis_index("wave"), lax.axis_index("lev")
    lat_total = z.bands * z.rows
    lev_total = z.sets * z.levels
    own = slice(halo, halo + z.levels)
    q_ref[...] = jnp.zeros_like(q_ref)
    f_ref[...] = jnp.zeros_like(f_ref)
    for j in range(halo):
        south, north = by_parity("wave", first_ref[j], second_ref[j])
        q_ref[j, own] = south
        q_ref[halo + z.rows + j, own] = north
    south, north = by_parity("wave", first_ref[z.rows], second_ref[z.rows])
    f_ref[0, own] = south
    f_ref[z.rows + 1, own] = north
    for j in range(z.rows):
        q_ref[halo + j, own] = own_ref[j]
        f_ref[1 + j, own] = own_ref[z.rows + j]
    below, above = by_parity("lev", lev_first_ref[...], lev_second_ref[...])
    for got, near, far in ((below, halo - 1, 0), (above, halo + z.levels, z.deep - 1)):
        for j in range(z.rows + 2):
            q_ref[halo - 1 + j, near : near + 1] = got[j : j + 1]
        for j in range(z.rows):
            at = z.rows + 2 + j
            q_ref[halo + j, far : far + 1] = got[at : at + 1]
            at = 2 * z.rows + 2 + j
            f_ref[1 + j, near : near + 1] = got[at : at + 1]

    height = z.bands * z.slot_pad

    def from_set(index):
        blocks = [arrived_ref[z.bands - 1 - b, z.sets - 1 - index] for b in range(z.bands)]
        return jnp.concatenate(blocks, axis=0)

    blocks = jnp.concatenate(
        [
            from_set(level_set),
            from_set(jnp.maximum(level_set - 1, 0)),
            from_set(jnp.minimum(level_set + 1, z.sets - 1)),
        ],
        axis=1,
    )
    turned = contract(unpack_ref[...], blocks, ((1,), (1,))).astype(jnp.bfloat16)
    span = turned.shape[0] // 2
    turned = jnp.concatenate([turned[:span], turned[span:]], axis=1)
    winds = contract(turned, table_ref[...], ((1,), (0,)))

    def wind(which, j):
        first = which * z.stack + j * z.deep
        return courant_limit * jnp.tanh(winds[first : first + z.deep])

    zonal = [wind(0, j) for j in range(1, z.rows + 3)]
    merid = [wind(1, j) for j in range(z.window)]

    def west(x):
        return pltpu.roll(x, 1, 1)

    def east(x):
        return pltpu.roll(x, z.lon - 1, 1)

    face = []
    for j in range(z.rows + 2):
        speed = 0.5 * (west(zonal[j]) + zonal[j])
        magnitude = jnp.abs(speed)
        diffuse = 0.5 * (magnitude - f_ref[j] * (magnitude - speed * speed))
        face.append((speed, diffuse))
    lat_face = []
    for j in range(1, z.window):
        index = band * z.rows - halo + j
        is_open = jnp.where((index > 0) & (index < lat_total), 0.5, 0.0).astype(jnp.float32)
        speed = 0.5 * (merid[j - 1] + merid[j])
        lat_face.append((speed * is_open, jnp.abs(speed) * is_open))
    deep = lax.broadcasted_iota(jnp.int32, (z.deep, z.lon), 0) + (level_set * z.levels - halo)
    rise = jnp.where((deep > 0) & (deep < lev_total), diffusivity, 0.0).astype(jnp.float32)

    def tendency(q, first):
        north_flux = []
        for j in range(len(q) - 1):
            mean, spread = lat_face[first - 1 + j]
            north_flux.append(mean * (q[j] + q[j + 1]) - spread * (q[j + 1] - q[j]))
        result = []
        for j in range(1, len(q) - 1):
            speed, diffuse = face[first - 2 + j]
            centre = q[j]
            western = west(centre)
            flux = speed * 0.5 * (western + centre) - diffuse * (centre - western)
            lift = rise * (centre - pltpu.roll(centre, 1, 0))
            result.append(
                -(east(flux) - flux)
                - (north_flux[j] - north_flux[j - 1])
                + (pltpu.roll(lift, z.deep - 1, 0) - lift)
            )
        return result

    tracer = [q_ref[j] for j in range(z.window)]
    first_tendency = tendency(tracer, 1)
    section_one = [q + t for q, t in zip(tracer[1:-1], first_tendency)]
    section_two = tendency(section_one, 2)
    tops, lows = [], []
    for j in range(z.rows):
        q = tracer[halo + j]
        change = 0.5 * q + 0.5 * (section_one[1 + j] + section_two[j]) - q
        top = change.astype(jnp.bfloat16)
        tops.append(top.astype(jnp.float32))
        lows.append(change - tops[-1])
    both = jnp.concatenate(tops + lows, axis=0).astype(jnp.bfloat16)
    projected = contract(both, table_ref[...], ((1,), (1,)))
    count = z.rows * z.deep
    projected = projected[:count] + projected[count:]
    scaled = projected * scale_ref[:, :1]
    top = scaled.astype(jnp.bfloat16)
    low = (scaled - top.astype(jnp.float32)).astype(jnp.bfloat16)
    both = jnp.concatenate([top, low], axis=0)

    def of_band(b):
        first = b * z.slot_pad
        halves = [both[:, p * height + first : p * height + first + z.slot_pad] for p in range(2)]
        return jnp.concatenate(halves, axis=1)

    spread = jnp.concatenate([of_band(b) for b in range(z.bands)], axis=0)
    spread = contract(spread, spread_ref[...], ((1,), (0,)))
    for b in range(z.bands):
        block = spread[2 * b * count : 2 * (b + 1) * count]
        block = block[:count] + block[count:]
        for j in range(z.rows):
            mine = block[j * z.deep : (j + 1) * z.deep] * pick_ref[...]
            reply_ref[z.order.index(b), j : j + 1] = jnp.sum(mine, axis=0, keepdims=True)


def analysis_kernel(z, arrived_ref, live_ref, out_hbm, turned_ref, out_ref, sems):
    arrived = [arrived_ref[z.order.index(b)] for b in range(z.bands)]
    arrived = jnp.concatenate(arrived, axis=0)
    top = arrived.astype(jnp.bfloat16).astype(jnp.float32)
    turned = jnp.concatenate([top, arrived - top], axis=0)
    width = turned_ref.shape[2]
    for c in range(turned_ref.shape[0]):
        turned_ref[c] = turned[c * width : (c + 1) * width].T
    height = 2 * z.levels
    stores = []
    for s in range(z.slots):
        left = [
            turned_ref[c, pl.ds(s, height, stride=z.slot_pad), :].astype(jnp.bfloat16)
            for c in range(turned_ref.shape[0])
        ]
        left = jnp.concatenate(left, axis=1)
        right = jnp.concatenate([live_ref[s], live_ref[s]], axis=0)
        out_ref[s] = contract(left, right, ((1,), (0,))).reshape(2, z.levels, z.degrees)
        if s % store_slots == store_slots - 1 or s == z.slots - 1:
            first = s // store_slots * store_slots
            part = pl.ds(first, s + 1 - first)
            stores.append(
                pltpu.make_async_copy(out_ref.at[part], out_hbm.at[part], sems.at[len(stores)])
            )
            stores[-1].start()
    for store in stores:
        store.wait()


def in_hbm(array):
    return pltpu.with_memory_space_constraint(array, pltpu.HBM)


def nbytes(array, dtype=None):
    return array.size * jnp.dtype(dtype or array.dtype).itemsize


def swaps(axis):
    count = lax.axis_size(axis)
    pairs = [[(i, i + 1) for i in range(start, count - 1, 2)] for start in (0, 1)]
    return [p + [(b, a) for a, b in p] for p in pairs]


def on_device(spectra, legendre, derivative, tracer, limiter_flags, lat_weight, slot_wave):
    z = Sizes(spectra, legendre, tracer, lax.axis_size("wave"), lax.axis_size("lev"))
    f32, bf16 = jnp.float32, jnp.bfloat16
    fan = 4 * z.bands * z.sets * z.slot_pad * z.piece
    table_bytes = 4 * z.bands * z.slot_pad * z.lon
    any_spec = pl.BlockSpec(memory_space=pltpu.HBM)
    edge_shape = jax.ShapeDtypeStruct((z.rows + 1, z.levels, z.lon), f32)
    group_count = -(-z.slots * z.unit // lanes)
    fetched = (slot_wave, lat_weight, spectra, legendre, derivative, tracer, limiter_flags)
    pieces, live, scale, own, to_first, to_second = pl.pallas_call(
        functools.partial(legendre_kernel, z),
        name="legendre",
        in_specs=[any_spec] * len(fetched),
        out_specs=tuple(vmem(6)),
        out_shape=(
            jax.ShapeDtypeStruct((z.bands * z.sets, z.slot_pad, z.piece), bf16),
            jax.ShapeDtypeStruct(legendre.shape, bf16),
            jax.ShapeDtypeStruct((z.rows * z.deep, lanes), f32),
            jax.ShapeDtypeStruct((2 * z.rows, z.levels, z.lon), f32),
            edge_shape,
            edge_shape,
        ),
        scratch_shapes=[pltpu.SMEM(x.shape, x.dtype) for x in fetched[:2]]
        + [pltpu.VMEM(x.shape, x.dtype) for x in fetched[2:]]
        + [
            pltpu.VMEM((z.slot_pad * z.lats, lanes), f32),
            pltpu.SemaphoreType.DMA((7, group_count)),
        ],
        compiler_params=params(
            2 * nbytes(spectra), 6 * nbytes(legendre), 8 * nbytes(tracer), fan
        ),
    )(*map(in_hbm, fetched))
    first_pairs, second_pairs = swaps("wave")
    wave_first = lax.ppermute(to_first, "wave", first_pairs)
    wave_second = lax.ppermute(to_second, "wave", second_pairs)
    arrived = lax.all_to_all(
        pieces,
        ("wave", "lev"),
        split_axis=0,
        concat_axis=0,
        axis_index_groups=[list(range(z.bands * z.sets))[::-1]],
        tiled=True,
    )
    padded_wave = jnp.pad(
        slot_wave.reshape(z.bands, z.slots), ((0, 0), (0, z.slot_pad - z.slots))
    ).reshape(-1, 1)
    table = pl.pallas_call(
        functools.partial(table_kernel, z),
        name="table",
        in_specs=vmem(1),
        out_specs=vmem(1)[0],
        out_shape=jax.ShapeDtypeStruct((2 * z.bands * z.slot_pad, z.lon), bf16),
        compiler_params=params(table_bytes),
    )(padded_wave)
    up_shape = jax.ShapeDtypeStruct((3 * z.rows + 2, z.lon), f32)
    up, down = pl.pallas_call(
        functools.partial(edge_kernel, z),
        name="edges",
        in_specs=vmem(3),
        out_specs=tuple(vmem(2)),
        out_shape=(up_shape, up_shape),
        compiler_params=params(8 * nbytes(tracer)),
    )(own, wave_first, wave_second)
    first_pairs, second_pairs = swaps("lev")
    lev_first = lax.ppermute(up, "lev", first_pairs)
    lev_second = lax.ppermute(down, "lev", second_pairs)
    reply = pl.pallas_call(
        functools.partial(grid_kernel, z),
        name="grid",
        in_specs=vmem(11),
        out_specs=vmem(1)[0],
        out_shape=jax.ShapeDtypeStruct((z.bands, z.rows, z.reply), f32),
        scratch_shapes=[
            pltpu.VMEM((z.window, z.deep, z.lon), f32),
            pltpu.VMEM((z.rows + 2, z.deep, z.lon), f32),
        ],
        compiler_params=params(3 * table_bytes, 24 * nbytes(tracer), fan),
    )(
        arrived.reshape(z.bands, z.sets, z.slot_pad, z.piece),
        unpack_constant(z),
        table,
        own,
        wave_first,
        wave_second,
        lev_first,
        lev_second,
        *reply_constants(z),
        scale,
    )
    returned = lax.all_to_all(
        reply, "wave", split_axis=0, concat_axis=0, axis_index_groups=[z.order], tiled=True
    )
    width = math.gcd(2 * z.lats, lanes)
    return pl.pallas_call(
        functools.partial(analysis_kernel, z),
        name="analysis",
        in_specs=vmem(2),
        out_specs=any_spec,
        out_shape=jax.ShapeDtypeStruct((z.slots, 2, z.levels, z.degrees), f32),
        scratch_shapes=[
            pltpu.VMEM((2 * z.lats // width, z.reply, width), f32),
            pltpu.VMEM((z.slots, 2, z.levels, z.degrees), f32),
            pltpu.SemaphoreType.DMA((-(-z.slots // store_slots),)),
        ],
        compiler_params=params(nbytes(spectra, f32), nbytes(legendre)),
    )(returned, live)


def solution(mesh):
    return jax.shard_map(
        on_device,
        mesh=mesh,
        in_specs=(
            P("wave", None, "lev", None),
            P("wave", None, None),
            P("wave", None, None),
            P("lev", "wave", None),
            P("lev", "wave", None),
            P("wave"),
            P(),
        ),
        out_specs=P("wave", None, "lev", None),
        check_vma=False,
    )
```

```python
import functools
import math

import jax
import jax.numpy as jnp
import numpy as np
from jax import lax
from jax.experimental import pallas as pl
from jax.experimental.pallas import tpu as pltpu
from jax.sharding import PartitionSpec as P

diffusivity = 0.15
courant_limit = 0.45
halo = 2
lanes = 128
packed_rows = 16
store_slots = 4


def round_up(value, step):
    return -(-value // step) * step


def contract(left, right, dims):
    return lax.dot_general(left, right, (dims, ((), ())), preferred_element_type=jnp.float32)


def vmem(count):
    return [pl.BlockSpec(memory_space=pltpu.VMEM)] * count


def params(*byte_counts):
    return pltpu.CompilerParams(vmem_limit_bytes=min(60 * 2**20, 6 * 2**20 + sum(byte_counts)))


class Sizes:
    def __init__(self, spectra, legendre, tracer, bands, sets):
        self.slots, _, self.levels, self.degrees = spectra.shape
        self.lats = legendre.shape[1]
        self.rows, self.lon = tracer.shape[1:]
        self.bands, self.sets = bands, sets
        self.order = [(bands // 2 + 1 - b) % bands for b in range(bands)]
        self.slot_pad = round_up(self.slots, packed_rows)
        self.window = self.rows + 2 * halo
        self.deep = self.levels + 2 * halo
        self.unit = 4 * self.levels
        self.piece = round_up(self.window * self.unit, lanes)
        self.stack = round_up(self.window * self.deep, 8)
        self.reply = round_up(2 * self.levels * self.slot_pad, lanes)
        assert self.rows == halo and self.deep == 8 and self.lon % lanes == 0
        assert lanes % self.unit == 0 and self.lats % 8 == 0


def piece_lanes(z):
    at = np.arange(z.piece)
    row, channel, level = at // z.unit, at // z.levels % 4, at % z.levels
    return channel % 2, channel // 2, row, level, row < z.window


def unpack_constant(z):
    part, wind, row, level, valid = piece_lanes(z)
    height = round_up(2 * z.stack, lanes)
    target = np.arange(2 * height)
    t_part, rest = target // height, target % height
    t_wind, rest = rest // z.stack, rest % z.stack
    t_row, t_deep = rest // z.deep, rest % z.deep
    t_valid = (t_wind < 2) & (t_row < z.window)
    same = (t_part[:, None] == part) & (t_wind[:, None] == wind) & (t_row[:, None] == row)
    same = same & valid & t_valid[:, None]
    own = same & (t_deep[:, None] == level + halo)
    below = same & (t_deep[:, None] == halo - 1) & (level == z.levels - 1)
    above = same & (t_deep[:, None] == halo + z.levels) & (level == 0)
    return jnp.asarray(np.concatenate([own, below, above], axis=1), jnp.bfloat16)


def reply_constants(z):
    at = np.arange(z.reply)
    part, rest = at // (z.levels * z.slot_pad), at % (z.levels * z.slot_pad)
    level, slot = rest // z.slot_pad, rest % z.slot_pad
    source = np.arange(2 * z.slot_pad)
    spread = (source[:, None] // z.slot_pad == part) & (source[:, None] % z.slot_pad == slot)
    pick = np.arange(z.deep)[:, None] == level + halo
    return jnp.asarray(spread, jnp.bfloat16), pick.astype(np.float32)


def legendre_kernel(
    z,
    wave_hbm,
    weight_hbm,
    spectra_hbm,
    legendre_hbm,
    derivative_hbm,
    tracer_hbm,
    flags_hbm,
    pieces_ref,
    live_ref,
    scale_ref,
    own_ref,
    first_ref,
    second_ref,
    wave_ref,
    weight_ref,
    spectra_ref,
    legendre_ref,
    derivative_ref,
    tracer_ref,
    flags_ref,
    by_slot_ref,
    sems,
):
    group_slots = lanes // z.unit
    groups = [
        (first, min(first + group_slots, z.slots)) for first in range(0, z.slots, group_slots)
    ]
    whole = [
        pltpu.make_async_copy(hbm, ref, sems.at[a, 0])
        for a, (hbm, ref) in enumerate(
            (
                (wave_hbm, wave_ref),
                (weight_hbm, weight_ref),
                (tracer_hbm, tracer_ref),
                (flags_hbm, flags_ref),
            )
        )
    ]
    fetches = [
        [
            pltpu.make_async_copy(hbm, ref, sems.at[4 + a, 0])
            for a, (hbm, ref) in enumerate(
                (
                    (spectra_hbm, spectra_ref),
                    (legendre_hbm, legendre_ref),
                    (derivative_hbm, derivative_ref),
                )
            )
        ]
    ] + [[] for _ in groups[1:]]
    for copies in [*fetches, whole]:
        for copy in copies:
            copy.start()
    base = lax.axis_index("wave") * z.slots
    by_slot_ref[...] = jnp.zeros_like(by_slot_ref)
    whole[0].wait()
    whole[1].wait()
    for j in range(z.rows):
        scale = weight_ref[j] * (1.0 / math.sqrt(z.lon))
        scale_ref[j * z.deep : (j + 1) * z.deep] = jnp.full((z.deep, lanes), scale, jnp.float32)
    degree = lax.broadcasted_iota(jnp.int32, (z.lats, z.degrees), 1)
    lane = lax.broadcasted_iota(jnp.int32, (z.lats, lanes), 1)
    lane_slot, channel = lane // z.unit, lane // z.levels % 4
    sign_sum = jnp.where(channel % 2 == 0, -1.0, 1.0)
    sign_slope = jnp.where(channel < 2, -1.0, 1.0)
    for (first, last), copies in zip(groups, fetches):
        waves = [wave_ref[base + s] for s in range(first, last)]
        for copy in copies:
            copy.wait()
        sums, slopes = [], []
        for s, wave in zip(range(first, last), waves):
            live = jnp.where(degree >= wave, 1.0, 0.0).astype(jnp.bfloat16)
            masked = legendre_ref[s] * live
            live_ref[s] = masked
            sums.append(masked)
            slopes.append(derivative_ref[s] * live)
        right = [spectra_ref[s].reshape(z.unit, z.degrees) for s in range(first, last)]
        right += [jnp.zeros_like(right[0])] * (group_slots - len(right))
        right = jnp.concatenate(right, axis=0)
        sums = contract(jnp.concatenate(sums, axis=0), right, ((1,), (1,)))
        slopes = contract(jnp.concatenate(slopes, axis=0), right, ((1,), (1,)))
        sum_of = jnp.zeros((z.lats, lanes), jnp.float32)
        slope_of = sum_of
        factor = sum_of
        doubled = sum_of
        for at, wave in enumerate(waves):
            mine = lane_slot == at
            block = slice(at * z.lats, (at + 1) * z.lats)
            sum_of = jnp.where(mine, sums[block], sum_of)
            slope_of = jnp.where(mine, slopes[block], slope_of)
            factor = jnp.where(mine, wave.astype(jnp.float32) / z.degrees, factor)
            doubled = jnp.where(mine, jnp.where(wave == 0, 1.0, 2.0), doubled)
        turned = sum_of
        for c in range(4):
            moved = pltpu.roll(sum_of, (2 * c - 3) * z.levels % lanes, 1)
            turned = jnp.where(channel == c, moved, turned)
        winds = (factor * sign_sum * turned + sign_slope * slope_of) * doubled
        for at, s in enumerate(range(first, last)):
            moved = winds if at == 0 else pltpu.roll(winds, lanes - at * z.unit, 1)
            by_slot_ref[s * z.lats : (s + 1) * z.lats] = moved
    tiles = round_up((z.lats + 2 * halo) * z.unit, lanes) // lanes + z.piece // lanes
    rows = [jnp.zeros((z.slot_pad, lanes), jnp.float32) for _ in range(tiles)]
    slot_lane = lax.broadcasted_iota(jnp.int32, (z.slot_pad, lanes), 1) // z.unit
    for lat in range(z.lats):
        tile, at = divmod((lat + halo) * z.unit, lanes)
        block = by_slot_ref[pl.ds(lat, z.slot_pad, stride=z.lats), :]
        block = block if at == 0 else pltpu.roll(block, at, 1)
        rows[tile] = jnp.where(slot_lane == at // z.unit, block, rows[tile])
    rows = jnp.concatenate(rows, axis=1)
    for b in range(z.bands):
        at = b * z.rows * z.unit
        piece = rows[:, at : at + z.piece].astype(jnp.bfloat16)
        for l in range(z.sets):
            pieces_ref[b * z.sets + z.sets - 1 - l] = piece

    even = lax.axis_index("wave") % 2 == 0
    whole[2].wait()
    for j in range(z.rows):
        row = tracer_ref[:, j, :]
        own_ref[j] = row
        first_ref[j] = row
        second_ref[j] = row
    whole[3].wait()
    switched = [flags_ref[:, j, :].astype(jnp.float32) for j in range(z.rows)]
    for j in range(z.rows):
        own_ref[z.rows + j] = switched[j]
    first_ref[z.rows] = jnp.where(even, switched[-1], switched[0])
    second_ref[z.rows] = jnp.where(even, switched[0], switched[-1])


def table_kernel(z, wave_ref, table_ref):
    wave = wave_ref[...].astype(jnp.float32)
    height = wave.shape[0]
    chunks = z.lon // lanes
    at = lax.broadcasted_iota(jnp.int32, (height, lanes), 1).astype(jnp.float32)

    def parts(phase):
        phase = phase - jnp.floor(phase * (1.0 / z.lon) + 0.5) * z.lon
        angle = phase * (2.0 * math.pi / z.lon)
        return jnp.cos(angle), jnp.sin(angle)

    fine_cos, fine_sin = parts(wave * at)
    coarse = [parts(wave * ((at + b) * lanes)) for b in range(0, chunks, lanes)]
    for a in range(chunks):
        cos_a = coarse[a // lanes][0][:, a % lanes : a % lanes + 1]
        sin_a = coarse[a // lanes][1][:, a % lanes : a % lanes + 1]
        columns = slice(a * lanes, (a + 1) * lanes)
        table_ref[:height, columns] = (cos_a * fine_cos - sin_a * fine_sin).astype(jnp.bfloat16)
        table_ref[height:, columns] = (-(sin_a * fine_cos + cos_a * fine_sin)).astype(jnp.bfloat16)


def by_parity(axis, first, second):
    even = lax.axis_index(axis) % 2 == 0
    return jnp.where(even, second, first), jnp.where(even, first, second)


def edge_kernel(z, own_ref, first_ref, second_ref, up_ref, down_ref):
    south, _ = by_parity("wave", first_ref[z.rows - 1], second_ref[z.rows - 1])
    _, north = by_parity("wave", first_ref[0], second_ref[0])
    even = lax.axis_index("lev") % 2 == 0
    rows = [south] + [own_ref[j] for j in range(z.rows)] + [north]
    plan = [(row, z.levels - 1, 0) for row in rows]
    plan += [(row, z.levels - 2, 1) for row in rows[1:-1]]
    plan += [(own_ref[z.rows + j], z.levels - 1, 0) for j in range(z.rows)]
    for at, (row, top, bottom) in enumerate(plan):
        top, bottom = row[top : top + 1], row[bottom : bottom + 1]
        up_ref[at : at + 1] = jnp.where(even, top, bottom)
        down_ref[at : at + 1] = jnp.where(even, bottom, top)


def grid_kernel(
    z,
    arrived_ref,
    unpack_ref,
    table_ref,
    own_ref,
    first_ref,
    second_ref,
    lev_first_ref,
    lev_second_ref,
    spread_ref,
    pick_ref,
    scale_ref,
    reply_ref,
    q_ref,
    f_ref,
):
    band, level_set = lax.axis_index("wave"), lax.axis_index("lev")
    lat_total = z.bands * z.rows
    lev_total = z.sets * z.levels
    own = slice(halo, halo + z.levels)
    q_ref[...] = jnp.zeros_like(q_ref)
    f_ref[...] = jnp.zeros_like(f_ref)
    for j in range(halo):
        south, north = by_parity("wave", first_ref[j], second_ref[j])
        q_ref[j, own] = south
        q_ref[halo + z.rows + j, own] = north
    south, north = by_parity("wave", first_ref[z.rows], second_ref[z.rows])
    f_ref[0, own] = south
    f_ref[z.rows + 1, own] = north
    for j in range(z.rows):
        q_ref[halo + j, own] = own_ref[j]
        f_ref[1 + j, own] = own_ref[z.rows + j]
    below, above = by_parity("lev", lev_first_ref[...], lev_second_ref[...])
    for got, near, far in ((below, halo - 1, 0), (above, halo + z.levels, z.deep - 1)):
        for j in range(z.rows + 2):
            q_ref[halo - 1 + j, near : near + 1] = got[j : j + 1]
        for j in range(z.rows):
            at = z.rows + 2 + j
            q_ref[halo + j, far : far + 1] = got[at : at + 1]
            at = 2 * z.rows + 2 + j
            f_ref[1 + j, near : near + 1] = got[at : at + 1]

    height = z.bands * z.slot_pad

    def from_set(index):
        blocks = [arrived_ref[b, z.sets - 1 - index] for b in range(z.bands)]
        return jnp.concatenate(blocks, axis=0)

    blocks = jnp.concatenate(
        [
            from_set(level_set),
            from_set(jnp.maximum(level_set - 1, 0)),
            from_set(jnp.minimum(level_set + 1, z.sets - 1)),
        ],
        axis=1,
    )
    turned = contract(unpack_ref[...], blocks, ((1,), (1,))).astype(jnp.bfloat16)
    span = turned.shape[0] // 2
    turned = jnp.concatenate([turned[:span], turned[span:]], axis=1)
    winds = contract(turned, table_ref[...], ((1,), (0,)))

    def wind(which, j):
        first = which * z.stack + j * z.deep
        return courant_limit * jnp.tanh(winds[first : first + z.deep])

    zonal = [wind(0, j) for j in range(1, z.rows + 3)]
    merid = [wind(1, j) for j in range(z.window)]

    def west(x):
        return pltpu.roll(x, 1, 1)

    def east(x):
        return pltpu.roll(x, z.lon - 1, 1)

    face = []
    for j in range(z.rows + 2):
        speed = 0.5 * (west(zonal[j]) + zonal[j])
        magnitude = jnp.abs(speed)
        diffuse = 0.5 * (magnitude - f_ref[j] * (magnitude - speed * speed))
        face.append((speed, diffuse))
    lat_face = []
    for j in range(1, z.window):
        index = band * z.rows - halo + j
        is_open = jnp.where((index > 0) & (index < lat_total), 0.5, 0.0).astype(jnp.float32)
        speed = 0.5 * (merid[j - 1] + merid[j])
        lat_face.append((speed * is_open, jnp.abs(speed) * is_open))
    deep = lax.broadcasted_iota(jnp.int32, (z.deep, z.lon), 0) + (level_set * z.levels - halo)
    rise = jnp.where((deep > 0) & (deep < lev_total), diffusivity, 0.0).astype(jnp.float32)

    def tendency(q, first):
        north_flux = []
        for j in range(len(q) - 1):
            mean, spread = lat_face[first - 1 + j]
            north_flux.append(mean * (q[j] + q[j + 1]) - spread * (q[j + 1] - q[j]))
        result = []
        for j in range(1, len(q) - 1):
            speed, diffuse = face[first - 2 + j]
            centre = q[j]
            western = west(centre)
            flux = speed * 0.5 * (western + centre) - diffuse * (centre - western)
            lift = rise * (centre - pltpu.roll(centre, 1, 0))
            result.append(
                -(east(flux) - flux)
                - (north_flux[j] - north_flux[j - 1])
                + (pltpu.roll(lift, z.deep - 1, 0) - lift)
            )
        return result

    tracer = [q_ref[j] for j in range(z.window)]
    first_tendency = tendency(tracer, 1)
    section_one = [q + t for q, t in zip(tracer[1:-1], first_tendency)]
    section_two = tendency(section_one, 2)
    tops, lows = [], []
    for j in range(z.rows):
        q = tracer[halo + j]
        change = 0.5 * q + 0.5 * (section_one[1 + j] + section_two[j]) - q
        top = change.astype(jnp.bfloat16)
        tops.append(top.astype(jnp.float32))
        lows.append(change - tops[-1])
    both = jnp.concatenate(tops + lows, axis=0).astype(jnp.bfloat16)
    projected = contract(both, table_ref[...], ((1,), (1,)))
    count = z.rows * z.deep
    projected = projected[:count] + projected[count:]
    scaled = projected * scale_ref[:, :1]
    top = scaled.astype(jnp.bfloat16)
    low = (scaled - top.astype(jnp.float32)).astype(jnp.bfloat16)
    both = jnp.concatenate([top, low], axis=0)

    def of_band(b):
        first = b * z.slot_pad
        halves = [both[:, p * height + first : p * height + first + z.slot_pad] for p in range(2)]
        return jnp.concatenate(halves, axis=1)

    spread = jnp.concatenate([of_band(b) for b in range(z.bands)], axis=0)
    spread = contract(spread, spread_ref[...], ((1,), (0,)))
    for b in range(z.bands):
        block = spread[2 * b * count : 2 * (b + 1) * count]
        block = block[:count] + block[count:]
        for j in range(z.rows):
            mine = block[j * z.deep : (j + 1) * z.deep] * pick_ref[...]
            reply_ref[z.order.index(b), j : j + 1] = jnp.sum(mine, axis=0, keepdims=True)


def analysis_kernel(z, arrived_ref, live_ref, out_hbm, turned_ref, out_ref, sems):
    arrived = [arrived_ref[z.order.index(b)] for b in range(z.bands)]
    arrived = jnp.concatenate(arrived, axis=0)
    top = arrived.astype(jnp.bfloat16).astype(jnp.float32)
    turned = jnp.concatenate([top, arrived - top], axis=0)
    width = turned_ref.shape[2]
    for c in range(turned_ref.shape[0]):
        turned_ref[c] = turned[c * width : (c + 1) * width].T
    height = 2 * z.levels
    stores = []
    for s in range(z.slots):
        left = [
            turned_ref[c, pl.ds(s, height, stride=z.slot_pad), :].astype(jnp.bfloat16)
            for c in range(turned_ref.shape[0])
        ]
        left = jnp.concatenate(left, axis=1)
        right = jnp.concatenate([live_ref[s], live_ref[s]], axis=0)
        out_ref[s] = contract(left, right, ((1,), (0,))).reshape(2, z.levels, z.degrees)
        if s % store_slots == store_slots - 1 or s == z.slots - 1:
            first = s // store_slots * store_slots
            part = pl.ds(first, s + 1 - first)
            stores.append(
                pltpu.make_async_copy(out_ref.at[part], out_hbm.at[part], sems.at[len(stores)])
            )
            stores[-1].start()
    for store in stores:
        store.wait()


def in_hbm(array):
    return pltpu.with_memory_space_constraint(array, pltpu.HBM)


def nbytes(array, dtype=None):
    return array.size * jnp.dtype(dtype or array.dtype).itemsize


def swaps(axis):
    count = lax.axis_size(axis)
    pairs = [[(i, i + 1) for i in range(start, count - 1, 2)] for start in (0, 1)]
    return [p + [(b, a) for a, b in p] for p in pairs]


def on_device(spectra, legendre, derivative, tracer, limiter_flags, lat_weight, slot_wave):
    z = Sizes(spectra, legendre, tracer, lax.axis_size("wave"), lax.axis_size("lev"))
    f32, bf16 = jnp.float32, jnp.bfloat16
    fan = 4 * z.bands * z.sets * z.slot_pad * z.piece
    table_bytes = 4 * z.bands * z.slot_pad * z.lon
    any_spec = pl.BlockSpec(memory_space=pltpu.HBM)
    edge_shape = jax.ShapeDtypeStruct((z.rows + 1, z.levels, z.lon), f32)
    group_count = -(-z.slots * z.unit // lanes)
    fetched = (slot_wave, lat_weight, spectra, legendre, derivative, tracer, limiter_flags)
    pieces, live, scale, own, to_first, to_second = pl.pallas_call(
        functools.partial(legendre_kernel, z),
        name="legendre",
        in_specs=[any_spec] * len(fetched),
        out_specs=tuple(vmem(6)),
        out_shape=(
            jax.ShapeDtypeStruct((z.bands * z.sets, z.slot_pad, z.piece), bf16),
            jax.ShapeDtypeStruct(legendre.shape, bf16),
            jax.ShapeDtypeStruct((z.rows * z.deep, lanes), f32),
            jax.ShapeDtypeStruct((2 * z.rows, z.levels, z.lon), f32),
            edge_shape,
            edge_shape,
        ),
        scratch_shapes=[pltpu.SMEM(x.shape, x.dtype) for x in fetched[:2]]
        + [pltpu.VMEM(x.shape, x.dtype) for x in fetched[2:]]
        + [
            pltpu.VMEM((z.slot_pad * z.lats, lanes), f32),
            pltpu.SemaphoreType.DMA((7, group_count)),
        ],
        compiler_params=params(
            2 * nbytes(spectra), 6 * nbytes(legendre), 8 * nbytes(tracer), fan
        ),
    )(*map(in_hbm, fetched))
    first_pairs, second_pairs = swaps("wave")
    wave_first = lax.ppermute(to_first, "wave", first_pairs)
    wave_second = lax.ppermute(to_second, "wave", second_pairs)
    arrived = lax.all_to_all(
        pieces,
        ("wave", "lev"),
        split_axis=0,
        concat_axis=0,
        axis_index_groups=[
            [b * z.sets + l for b in range(z.bands) for l in reversed(range(z.sets))]
        ],
        tiled=True,
    )
    padded_wave = jnp.pad(
        slot_wave.reshape(z.bands, z.slots), ((0, 0), (0, z.slot_pad - z.slots))
    ).reshape(-1, 1)
    table = pl.pallas_call(
        functools.partial(table_kernel, z),
        name="table",
        in_specs=vmem(1),
        out_specs=vmem(1)[0],
        out_shape=jax.ShapeDtypeStruct((2 * z.bands * z.slot_pad, z.lon), bf16),
        compiler_params=params(table_bytes),
    )(padded_wave)
    up_shape = jax.ShapeDtypeStruct((3 * z.rows + 2, z.lon), f32)
    up, down = pl.pallas_call(
        functools.partial(edge_kernel, z),
        name="edges",
        in_specs=vmem(3),
        out_specs=tuple(vmem(2)),
        out_shape=(up_shape, up_shape),
        compiler_params=params(8 * nbytes(tracer)),
    )(own, wave_first, wave_second)
    first_pairs, second_pairs = swaps("lev")
    lev_first = lax.ppermute(up, "lev", first_pairs)
    lev_second = lax.ppermute(down, "lev", second_pairs)
    reply = pl.pallas_call(
        functools.partial(grid_kernel, z),
        name="grid",
        in_specs=vmem(11),
        out_specs=vmem(1)[0],
        out_shape=jax.ShapeDtypeStruct((z.bands, z.rows, z.reply), f32),
        scratch_shapes=[
            pltpu.VMEM((z.window, z.deep, z.lon), f32),
            pltpu.VMEM((z.rows + 2, z.deep, z.lon), f32),
        ],
        compiler_params=params(3 * table_bytes, 24 * nbytes(tracer), fan),
    )(
        arrived.reshape(z.bands, z.sets, z.slot_pad, z.piece),
        unpack_constant(z),
        table,
        own,
        wave_first,
        wave_second,
        lev_first,
        lev_second,
        *reply_constants(z),
        scale,
    )
    returned = lax.all_to_all(
        reply, "wave", split_axis=0, concat_axis=0, axis_index_groups=[z.order], tiled=True
    )
    width = math.gcd(2 * z.lats, lanes)
    return pl.pallas_call(
        functools.partial(analysis_kernel, z),
        name="analysis",
        in_specs=vmem(2),
        out_specs=any_spec,
        out_shape=jax.ShapeDtypeStruct((z.slots, 2, z.levels, z.degrees), f32),
        scratch_shapes=[
            pltpu.VMEM((2 * z.lats // width, z.reply, width), f32),
            pltpu.VMEM((z.slots, 2, z.levels, z.degrees), f32),
            pltpu.SemaphoreType.DMA((-(-z.slots // store_slots),)),
        ],
        compiler_params=params(nbytes(spectra, f32), nbytes(legendre)),
    )(returned, live)


def solution(mesh):
    return jax.shard_map(
        on_device,
        mesh=mesh,
        in_specs=(
            P("wave", None, "lev", None),
            P("wave", None, None),
            P("wave", None, None),
            P("lev", "wave", None),
            P("lev", "wave", None),
            P("wave"),
            P(),
        ),
        out_specs=P("wave", None, "lev", None),
        check_vma=False,
    )
```
